128 devices in a mesh: seq: 64 (over x, z, y), head: 2 (over core).
Axes of the slice: x: 4, y: 4, z: 4, core: 2. Of those that a mesh axis runs over, the one named last changes fastest.
Arguments:
- queries: bfloat16 [16384, 4096], P('seq', 'head'), may hold values from -210 to 210
- keys: bfloat16 [16384, 1024], P('seq', 'head'), may hold values from -7 to 7
- values: bfloat16 [16384, 1024], P('seq', 'head'), may hold values from -6 to 6
- vertical: int32 [8, 64], P('head'), may hold values from 0 to 255, as said below
- slash: int32 [8, 2], P('head'), may hold values from 1 to 4, as said below
- out_weight: bfloat16 [4096, 4096], P('head'), may hold values from -1 to 1
Outputs:
- mixed: bfloat16 [16384, 4096], P(('seq', 'head'))
The draws below stay inside these ranges and needn't reach their ends.
Inputs may be any that keep to these rules, and one draw needn't show every extreme that they name: `vertical`: for each key-value head, 64 different key blocks in increasing order; block b lies in slab b // 4; no slab holds more than 2 of one head's blocks, and for every head some slab holds exactly 2. `slash`: for each key-value head, 2 different offsets in increasing order; some head has the offset 256 // 64.
All inputs are finite; a program needn't handle non-finite values.
Results may differ from the reference program's by a relative error of at most 0.01.
Values may be sent and summed in bfloat16 or wider, within the bound.
No kernel may reach another device: no remote copies, remote signals or barrier semaphores. Data moves between devices by JAX's collectives and lax.ppermute only.
A program may use at most 128 MiB of HBM per device.

```python
from functools import partial
import jax
import jax.numpy as jnp
from jax import lax

HEADS = 32
KEY_VALUE_HEADS = 8
HEAD_DIM = 128
DMODEL = 4096
S_DEV = 256
BLK = 64
NS = 2
CAP = 2
NV = 64
SEQ = 16384
N_SEQ = 64


def paired(key):
    key_seed, query_seed = jax.random.split(jax.random.fold_in(key, 7), 2)
    keys_f = jnp.clip(jax.random.normal(key_seed, (SEQ, KEY_VALUE_HEADS * HEAD_DIM), jnp.float32), -6.0, 6.0)
    query_f = jnp.clip(1.5 * jax.random.normal(query_seed, (SEQ, HEADS * HEAD_DIM), jnp.float32), -9.0, 9.0)
    return (query_f, keys_f)


def draw_queries(key, part):
    return paired(key)[0].astype(jnp.bfloat16)


def draw_keys(key, part):
    return paired(key)[1].astype(jnp.bfloat16)


def draw_vertical(key, part):
    block_span = S_DEV // BLK
    owners = SEQ // S_DEV
    perm_seed, score_seed, force_seed = jax.random.split(jax.random.fold_in(key, 3), 3)
    within = jax.random.randint(perm_seed, (KEY_VALUE_HEADS, owners, block_span), 0, 1 << 20) * block_span + jnp.arange(block_span, dtype=jnp.int32)
    order = jnp.argsort(within, axis=-1)[:, :, :CAP]
    blocks = (order + jnp.arange(owners, dtype=jnp.int32)[None, :, None] * block_span).reshape(KEY_VALUE_HEADS, owners * CAP)
    owner_of = jnp.repeat(jnp.arange(owners, dtype=jnp.int32), CAP)
    forced_blocks = jax.random.randint(force_seed, (KEY_VALUE_HEADS, 1), 0, owners)
    block_score = jax.random.randint(score_seed, (KEY_VALUE_HEADS, owners * CAP), 0, 4096) + (owners - owner_of)[None, :] * (8192 // owners)
    block_score = block_score + jnp.where(owner_of[None, :] == forced_blocks, 1 << 16, 0)
    block_score = block_score * (owners * CAP) + jnp.arange(owners * CAP, dtype=jnp.int32)[None, :]
    unused, picked = lax.top_k(block_score, NV)
    chosen = jnp.take_along_axis(blocks, picked, axis=1)
    return jnp.sort(chosen, axis=1).astype(jnp.int32)


def draw_slash(key, part):
    block_span = S_DEV // BLK
    score_seed, force_seed = jax.random.split(jax.random.fold_in(key, 5), 2)
    block_score = jax.random.randint(score_seed, (KEY_VALUE_HEADS, block_span), 0, 4096) * block_span + jnp.arange(block_span, dtype=jnp.int32)[None, :]
    forced_blocks = jax.random.randint(force_seed, (), 0, KEY_VALUE_HEADS)
    extra_score = (jnp.arange(KEY_VALUE_HEADS)[:, None] == forced_blocks) & (jnp.arange(block_span)[None, :] == block_span - 1)
    block_score = block_score + jnp.where(extra_score, 1 << 24, 0)
    unused, picked = lax.top_k(block_score, NS)
    return jnp.sort(picked + 1, axis=1).astype(jnp.int32)


def block_scale(key, shape, pieces, least, top_value):
    def one(position, blocks):
        steps = jax.random.uniform(jax.random.fold_in(jax.random.fold_in(key, 6), position), (blocks,), jnp.float32, least / len(pieces), top_value / len(pieces))
        return jnp.repeat(jnp.exp(steps), shape[position] // blocks).reshape((-1,) + (1,) * (len(shape) - position - 1))

    loudness = one(*pieces[0])
    for cut in pieces[1:]:
        loudness = loudness * one(*cut)
    return loudness


def bell_draw(key, shape, scale, bound, pieces=(), held_as=jnp.bfloat16):
    factor_of = block_scale(key, shape, pieces, -0.22, 0.18) if pieces else 1.0
    array = jax.random.normal(key, shape, jnp.float32) * scale * factor_of
    return jnp.minimum(jnp.maximum(array, -bound), bound).astype(held_as)


def setup_inputs(seed: int = 0) -> dict:
    splits = jax.random.split(jax.random.key(seed), 7)
    return {
        "queries": draw_queries(jax.random.fold_in(splits[6], 71), 0),
        "keys": draw_keys(jax.random.fold_in(splits[6], 71), 0),
        "values": bell_draw(splits[2], (SEQ, KEY_VALUE_HEADS * HEAD_DIM), 1.0, 6.0, ((0, 64), (1, 2))),
        "vertical": draw_vertical(jax.random.fold_in(splits[6], 71), 0),
        "slash": draw_slash(jax.random.fold_in(splits[6], 71), 0),
        "out_weight": bell_draw(splits[5], (HEADS * HEAD_DIM, DMODEL), HEADS ** -0.5, 1.0, ((0, 2),)),
    }


NEGATIVE = -1e30


def attended_block_tile(block_index, vert_ids, slash_ids, key_head, value_head, query_head_index, causal):
    offsets = jnp.concatenate([jnp.zeros((1,), jnp.int32), slash_ids.astype(jnp.int32)])
    diagonal = block_index - offsets
    vert_ok = (vert_ids < block_index) & jnp.all(block_index - vert_ids[:, None] != slash_ids[None, :], axis=1)
    diag_ok = diagonal >= 0
    chosen = jnp.concatenate([vert_ids.astype(jnp.int32), jnp.maximum(diagonal, 0).astype(jnp.int32)])
    usable = jnp.concatenate([vert_ok, diag_ok])
    gathered_keys = key_head[chosen].reshape(-1, HEAD_DIM)
    gathered_values = value_head[chosen].reshape(-1, HEAD_DIM)
    same_block = chosen == block_index
    allowed = usable[None, :, None] & (jnp.logical_not(same_block)[None, :, None] | causal[:, None, :])
    allowed = allowed.reshape(BLK, -1)
    query_block_tile = query_head_index[block_index]
    scores = jnp.einsum("qgd,kd->gqk", query_block_tile.astype(jnp.float32), gathered_keys.astype(jnp.float32)) * (HEAD_DIM ** -0.5)
    scores = jnp.where(allowed[None], scores, NEGATIVE)
    top_score = jnp.max(scores, axis=-1, keepdims=True)
    weights = jnp.where(allowed[None], jnp.exp(scores - top_score), 0.0)
    sum_weight = jnp.sum(weights, axis=-1, keepdims=True)
    rounded = lax.optimization_barrier(weights.astype(jnp.bfloat16)).astype(jnp.float32)
    output = jnp.einsum("gqk,kd->gqd", rounded, gathered_values.astype(jnp.float32)) / sum_weight
    return output.transpose(1, 0, 2).astype(jnp.bfloat16)


def attend_slab(slab_start, block_fn, slab_blocks):
    return jax.vmap(block_fn)(slab_start + jnp.arange(slab_blocks, dtype=jnp.int32))


def reference(queries, keys, values, vertical, slash, out_weight):
    per_group = HEADS // KEY_VALUE_HEADS
    block_count = SEQ // BLK
    slab_blocks = S_DEV // BLK
    query_blocks = queries.reshape(block_count, BLK, KEY_VALUE_HEADS, per_group, HEAD_DIM)
    key_blocks = keys.reshape(block_count, BLK, KEY_VALUE_HEADS, HEAD_DIM)
    value_blocks = values.reshape(block_count, BLK, KEY_VALUE_HEADS, HEAD_DIM)
    within = jnp.arange(BLK)
    causal = within[None, :] <= within[:, None]
    results = []
    for head_index in range(KEY_VALUE_HEADS):
        block_fn = partial(attended_block_tile, vert_ids=vertical[head_index], slash_ids=slash[head_index],
                           key_head=key_blocks[:, :, head_index], value_head=value_blocks[:, :, head_index],
                           query_head_index=query_blocks[:, :, head_index], causal=causal)
        mapped = lax.map(partial(attend_slab, block_fn=block_fn, slab_blocks=slab_blocks),
                         jnp.arange(N_SEQ, dtype=jnp.int32) * slab_blocks)
        results.append(mapped.reshape(SEQ, per_group * HEAD_DIM))
    attention = jnp.concatenate(results, axis=1)
    return jnp.dot(attention, out_weight, preferred_element_type=jnp.float32).astype(jnp.bfloat16)
```

```python
import functools

import jax
import jax.numpy as jnp
from jax import lax
from jax.experimental import pallas as pl
from jax.experimental.pallas import tpu as pltpu
from jax.sharding import Mesh
from jax.sharding import PartitionSpec as P

HEAD_DIM = 128
BLK = 64
SLAB = 256
NV = 64
EXP2_SCALE = HEAD_DIM ** (-0.5) * 1.4426950408889634
NEGATIVE = -1e30
ALL = ("x", "z", "y", "c")
MIB = 1 << 20


def moved(value, target):
    pairs = []
    for x in range(4):
        for z in range(4):
            for y in range(4):
                for c in range(2):
                    tx, tz, ty, tc = target(x, z, y, c)
                    pairs.append((((x * 4 + z) * 4 + y) * 2 + c, (((tx % 4) * 4 + tz % 4) * 4 + ty % 4) * 2 + tc))
    return lax.ppermute(value, ALL, pairs)


def along_y(value, by):
    return moved(value, lambda x, z, y, c: (x, z, y + by, c))


def first_hop(value, by):
    return moved(value, lambda x, z, y, c: (x + by, z, y, c) if c == 0 else (x, z + by, y, c))


def second_hop(value, by):
    return moved(value, lambda x, z, y, c: (x, z + by, y, c) if c == 0 else (x + by, z, y, c))


def to_next_group(value):
    return moved(value, lambda x, z, y, c: (x + (z + 1) // 4, z + 1, y, c))


def to_partner(value):
    return moved(value, lambda x, z, y, c: (x, z, y, 1 - c))


def rank_of(vert_ref, head, block):
    at = jnp.int32(0)
    for width in (32, 16, 8, 4, 2, 1):
        at = at + jnp.where(vert_ref[head, at + width - 1] < block, width, 0)
    return at + jnp.where(vert_ref[head, at] < block, 1, 0)


def slots_kernel(place_ref, vert_ref, keys_ref, values_ref, *slot_refs):
    group, y = place_ref[0], place_ref[1]
    first = (group * 4 + y) * 4
    for by in range(4):
        head = (y + by) % 4
        lanes = pl.ds(pl.multiple_of(head * HEAD_DIM, HEAD_DIM), HEAD_DIM)
        at = rank_of(vert_ref, head, first)
        for slot in range(2):
            entry = jnp.minimum(at + slot, NV - 1)
            block = vert_ref[head, entry] - first
            block = jnp.where((block >= 0) & (block < 4), block, 0)
            rows = pl.ds(pl.multiple_of(block * BLK, BLK), BLK)
            slot_refs[by][slot * BLK : (slot + 1) * BLK, :] = keys_ref[rows, lanes]
            slot_refs[by][128 + slot * BLK : 128 + (slot + 1) * BLK, :] = values_ref[rows, lanes]


def split_kernel(place_ref, queries_ref, keys_ref, values_ref, *out_refs):
    y = place_ref[1]
    for by in range(4):
        head = (y + by) % 4
        lanes = pl.ds(pl.multiple_of(head * HEAD_DIM, HEAD_DIM), HEAD_DIM)
        out_refs[by][:, 0:512] = queries_ref[:, pl.ds(pl.multiple_of(head * 512, 512), 512)]
        out_refs[by][:, 512:640] = keys_ref[:, lanes]
        out_refs[by][:, 640:768] = values_ref[:, lanes]


CHUNK = 1024


def attend(q, keys, values, allowed, top_ref, sum_ref, acc_ref):
    scores = lax.dot_general(q, keys, (((1,), (1,)), ((), ())), preferred_element_type=jnp.float32)
    if allowed is not None:
        scores = jnp.where(allowed, scores, NEGATIVE)
    old = top_ref[...]
    new = jnp.maximum(old, jnp.max(scores, axis=1, keepdims=True))
    shrink = jnp.exp2((old - new) * EXP2_SCALE)
    weights = jnp.exp2((scores - new[:, :1]) * EXP2_SCALE)
    part = weights[:, 0:128]
    for t in range(1, keys.shape[0] // 128):
        part = part + weights[:, 128 * t : 128 * (t + 1)]
    top_ref[...] = new
    sum_ref[...] = sum_ref[...] * shrink + part
    acc_ref[...] = acc_ref[...] * shrink + lax.dot_general(
        weights.astype(jnp.bfloat16), values, (((1,), (0,)), ((), ())), preferred_element_type=jnp.float32
    )


def attention_kernel(
    place_ref, vert_ref, slash_ref, q0, q1, q2, q3, prev_ref, g0, g1, g2, g3,
    o0, o1, o2, o3, kc, vc, kl, vl, ql, ol, top_ref, sum_ref, acc_ref,
):
    group, y, mine1, mine2, core = (place_ref[i] for i in range(5))
    qkv = (q0, q1, q2, q3)
    gathered = (g0, g1, g2, g3)
    outs = (o0, o1, o2, o3)
    head = y
    kl[0:SLAB, :] = prev_ref[:, 0:128]
    vl[0:SLAB, :] = prev_ref[:, 128:256]
    for by in range(4):
        slab = (y - by + 4) % 4
        rows = pl.ds(pl.multiple_of(SLAB + slab * SLAB, SLAB), SLAB)
        kl[rows, :] = qkv[by][:, 512:640]
        vl[rows, :] = qkv[by][:, 640:768]
        for block in range(4):
            for g in range(4):
                ql[by * 4 + block, g * BLK : (g + 1) * BLK, :] = qkv[by][
                    block * BLK : (block + 1) * BLK, g * 128 : (g + 1) * 128
                ]

    def compact(entry, last):
        block = vert_ref[head, entry]
        slab = block // 4
        rank = jnp.where(slab == last, 1, 0)
        x, z = slab // 16, (slab // 4) % 4
        first = jnp.where(core == 0, x, z)
        second = jnp.where(core == 0, z, x)
        inner = (mine1 - first + 4) % 4
        outer = (mine2 - second + 4) % 4
        by = (y - slab % 4 + 4) % 4
        row = (inner * 4 + by) * 256 + rank * BLK
        to = pl.ds(pl.multiple_of(entry * BLK, BLK), BLK)
        for i in range(4):
            @pl.when(outer == i)
            def _():
                kc[to, :] = gathered[i][pl.ds(pl.multiple_of(row, BLK), BLK), :]
                vc[to, :] = gathered[i][pl.ds(pl.multiple_of(row + 128, BLK), BLK), :]
        return slab

    lax.fori_loop(0, NV, compact, jnp.int32(-1))

    def one_block(i, carry):
        by, inside = i // 4, i % 4
        slab = (y - by + 4) % 4
        local = slab * 4 + inside
        block = group * 16 + local
        q = ql[i]
        top_ref[...] = jnp.full(top_ref.shape, NEGATIVE, jnp.float32)
        sum_ref[...] = jnp.zeros_like(sum_ref)
        acc_ref[...] = jnp.zeros_like(acc_ref)
        starts, valid = [local], []
        for s in range(2):
            offset = slash_ref[head, s]
            behind = block - offset
            at = jnp.minimum(rank_of(vert_ref, head, behind), NV - 1)
            ok = (behind >= 0) & (vert_ref[head, at] != behind)
            valid.append(jnp.where(ok, 1, 0))
            starts.append(local - offset)
        rows = [pl.ds(pl.multiple_of(SLAB + at * BLK, BLK), BLK) for at in starts]
        keys = jnp.concatenate([kl[r, :] for r in rows] + [kl[rows[0], :]], axis=0)
        values = jnp.concatenate([vl[r, :] for r in rows] + [vl[rows[0], :]], axis=0)
        column = lax.broadcasted_iota(jnp.int32, (256, 256), 1)
        row = lax.broadcasted_iota(jnp.int32, (256, 256), 0) % BLK
        limit = jnp.where(column < 64, row, jnp.where(column < 128, valid[0] * 256, jnp.where(column < 192, valid[1] * 256, 0)))
        attend(q, keys, values, column <= limit - jnp.where(column < 64, 0, 1), top_ref, sum_ref, acc_ref)
        count = rank_of(vert_ref, head, block) * BLK
        whole = count // CHUNK

        def full(n, carry):
            at = pl.ds(pl.multiple_of(n * CHUNK, CHUNK), CHUNK)
            attend(q, kc[at, :], vc[at, :], None, top_ref, sum_ref, acc_ref)
            return carry

        lax.fori_loop(0, whole, full, 0)

        @pl.when(count > whole * CHUNK)
        def _():
            at = pl.ds(pl.multiple_of(whole * CHUNK, CHUNK), CHUNK)
            column = lax.broadcasted_iota(jnp.int32, (256, CHUNK), 1)
            attend(q, kc[at, :], vc[at, :], column < count - whole * CHUNK, top_ref, sum_ref, acc_ref)

        total = jnp.sum(sum_ref[...], axis=1, keepdims=True)
        ol[i] = (acc_ref[...] / total).astype(jnp.bfloat16)
        return carry

    lax.fori_loop(0, 16, one_block, 0)
    for by in range(4):
        for block in range(4):
            for g in range(4):
                outs[by][block * BLK : (block + 1) * BLK, g * 128 : (g + 1) * 128] = ol[
                    by * 4 + block, g * BLK : (g + 1) * BLK, :
                ]


def project_kernel(place_ref, a0, a1, a2, a3, weight_ref, theirs_ref, mine_ref):
    y, core = place_ref[1], place_ref[4]
    total = None
    for by, a in enumerate((a0, a1, a2, a3)):
        head = (y + by) % 4
        rows = pl.ds(pl.multiple_of(head * 512, 512), 512)
        part = jnp.dot(a[...], weight_ref[rows, :], preferred_element_type=jnp.float32)
        total = part if total is None else total + part

    @pl.when(core == 0)
    def _():
        mine_ref[...] = total[0:128]
        theirs_ref[...] = total[128:256].astype(jnp.bfloat16)

    @pl.when(core == 1)
    def _():
        mine_ref[...] = total[128:256]
        theirs_ref[...] = total[0:128].astype(jnp.bfloat16)


SMEM = pl.BlockSpec(memory_space=pltpu.SMEM)
VMEM = pl.BlockSpec(memory_space=pltpu.VMEM)


def bf16(*shape):
    return jax.ShapeDtypeStruct(shape, jnp.bfloat16)


def params(limit):
    return pltpu.CompilerParams(vmem_limit_bytes=limit * MIB)


def cost(flops, moved_bytes):
    return pl.CostEstimate(flops=flops, bytes_accessed=moved_bytes, transcendentals=0)


def on_device(queries, keys, values, vertical, slash, out_weight):
    x, z, y, c = (lax.axis_index(a) for a in ALL)
    place = jnp.stack([x * 4 + z, y, jnp.where(c == 0, x, z), jnp.where(c == 0, z, x), c]).astype(jnp.int32)
    slots = pl.pallas_call(
        slots_kernel,
        out_shape=[bf16(256, 128)] * 4,
        in_specs=[SMEM, SMEM, VMEM, VMEM],
        out_specs=[VMEM] * 4,
        compiler_params=params(4),
        cost_estimate=cost(10**6, 10**6),
        name="slots",
    )(place, vertical, keys, values)
    slots = [slots[0]] + [along_y(slots[by], by) for by in (1, 2, 3)]
    own = jnp.concatenate(slots, axis=0)
    split = pl.pallas_call(
        split_kernel,
        out_shape=[bf16(256, 768)] * 4,
        in_specs=[SMEM, VMEM, VMEM, VMEM],
        out_specs=[VMEM] * 4,
        compiler_params=params(8),
        cost_estimate=cost(10**6, 3 * 10**6),
        name="split",
    )(place, queries, keys, values)
    qkv = [split[0]] + [along_y(split[by], by) for by in (1, 2, 3)]
    near = jnp.concatenate([own] + [first_hop(own, by) for by in (1, 2, 3)], axis=0)
    gathered = [near] + [second_hop(near, by) for by in (1, 2, 3)]
    last_slab = lax.select_n((y + 1) % 4, *[a[:, 512:768] for a in qkv])
    prev = to_next_group(last_slab)
    attention = pl.pallas_call(
        attention_kernel,
        out_shape=[bf16(256, 512)] * 4,
        in_specs=[SMEM] * 3 + [VMEM] * 9,
        out_specs=[VMEM] * 4,
        scratch_shapes=[
            pltpu.VMEM((NV * BLK, 128), jnp.bfloat16),
            pltpu.VMEM((NV * BLK, 128), jnp.bfloat16),
            pltpu.VMEM((5 * SLAB, 128), jnp.bfloat16),
            pltpu.VMEM((5 * SLAB, 128), jnp.bfloat16),
            pltpu.VMEM((16, 256, 128), jnp.bfloat16),
            pltpu.VMEM((16, 256, 128), jnp.bfloat16),
            pltpu.VMEM((256, 128), jnp.float32),
            pltpu.VMEM((256, 128), jnp.float32),
            pltpu.VMEM((256, 128), jnp.float32),
        ],
        compiler_params=params(28),
        cost_estimate=cost(2 * 10**10, 8 * 10**6),
        name="attention",
    )(place, vertical, slash, *qkv, prev, *gathered)
    back = [attention[0]] + [along_y(attention[by], -by) for by in (1, 2, 3)]
    columns = 512
    theirs, mine = pl.pallas_call(
        project_kernel,
        grid=(4096 // columns,),
        out_shape=[bf16(128, 4096), jax.ShapeDtypeStruct((128, 4096), jnp.float32)],
        in_specs=[SMEM] + [pl.BlockSpec((256, 512), lambda i: (0, 0))] * 4 + [pl.BlockSpec((2048, columns), lambda i: (0, i))],
        out_specs=[pl.BlockSpec((128, columns), lambda i: (0, i))] * 2,
        compiler_params=params(16),
        cost_estimate=cost(2 * 256 * 2048 * 4096, 2 * 10**7),
        name="project",
    )(place, *back, out_weight)
    return (mine + to_partner(theirs).astype(jnp.float32)).astype(jnp.bfloat16)


def solution(mesh):
    torus = Mesh(mesh.devices.reshape(4, 4, 4, 2), ALL)
    rows = ("x", "z", "y")
    placed = (P(rows, "c"), P(rows, "c"), P(rows, "c"), P("c", None), P("c", None), P("c", None))
    return jax.shard_map(on_device, mesh=torus, in_specs=placed, out_specs=P(ALL, None), check_vma=False)
```

```python
import functools

import jax
import jax.numpy as jnp
from jax import lax
from jax.experimental import pallas as pl
from jax.experimental.pallas import tpu as pltpu
from jax.sharding import Mesh
from jax.sharding import PartitionSpec as P

HEAD_DIM = 128
BLK = 64
SLAB = 256
NV = 64
EXP2_SCALE = HEAD_DIM ** (-0.5) * 1.4426950408889634
NEGATIVE = -1e30
ALL = ("x", "z", "y", "c")
MIB = 1 << 20


def moved(value, target):
    pairs = []
    for x in range(4):
        for z in range(4):
            for y in range(4):
                for c in range(2):
                    tx, tz, ty, tc = target(x, z, y, c)
                    pairs.append((((x * 4 + z) * 4 + y) * 2 + c, (((tx % 4) * 4 + tz % 4) * 4 + ty % 4) * 2 + tc))
    return lax.ppermute(value, ALL, pairs)


def along_y(value, by):
    return moved(value, lambda x, z, y, c: (x, z, y + by, c))


def first_hop(value, by):
    return moved(value, lambda x, z, y, c: (x + by, z, y, c) if c == 0 else (x, z + by, y, c))


def second_hop(value, by):
    return moved(value, lambda x, z, y, c: (x, z + by, y, c) if c == 0 else (x + by, z, y, c))


def to_next_group(value):
    return moved(value, lambda x, z, y, c: (x + (z + 1) // 4, z + 1, y, c))


def to_partner(value):
    return moved(value, lambda x, z, y, c: (x, z, y, 1 - c))


def rank_of(vert_ref, head, block):
    at = jnp.int32(0)
    for width in (32, 16, 8, 4, 2, 1):
        at = at + jnp.where(vert_ref[head, at + width - 1] < block, width, 0)
    return at + jnp.where(vert_ref[head, at] < block, 1, 0)


def slots_kernel(place_ref, vert_hbm, keys_hbm, values_hbm, *refs):
    slot_refs, (vert_ref, keys_ref, values_ref, sems) = refs[:4], refs[4:]
    copies = [
        pltpu.make_async_copy(vert_hbm, vert_ref, sems.at[0]),
        pltpu.make_async_copy(keys_hbm, keys_ref, sems.at[1]),
        pltpu.make_async_copy(values_hbm, values_ref, sems.at[2]),
    ]
    for copy in copies:
        copy.start()
    group, y = place_ref[0], place_ref[1]
    first = (group * 4 + y) * 4
    copies[0].wait()
    places = []
    for by in range(4):
        head = (y + by) % 4
        at = rank_of(vert_ref, head, first)
        for slot in range(2):
            entry = jnp.minimum(at + slot, NV - 1)
            block = vert_ref[head, entry] - first
            block = jnp.where((block >= 0) & (block < 4), block, 0)
            places.append(pl.ds(pl.multiple_of(block * BLK, BLK), BLK))
    copies[1].wait()
    copies[2].wait()
    for by in range(4):
        head = (y + by) % 4
        lanes = pl.ds(pl.multiple_of(head * HEAD_DIM, HEAD_DIM), HEAD_DIM)
        for slot in range(2):
            rows = places[by * 2 + slot]
            slot_refs[by][slot * BLK : (slot + 1) * BLK, :] = keys_ref[rows, lanes]
            slot_refs[by][128 + slot * BLK : 128 + (slot + 1) * BLK, :] = values_ref[rows, lanes]


def split_kernel(place_ref, queries_ref, keys_ref, values_ref, *out_refs):
    y = place_ref[1]
    for by in range(4):
        head = (y + by) % 4
        lanes = pl.ds(pl.multiple_of(head * HEAD_DIM, HEAD_DIM), HEAD_DIM)
        out_refs[by][:, 0:512] = queries_ref[:, pl.ds(pl.multiple_of(head * 512, 512), 512)]
        out_refs[by][:, 512:640] = keys_ref[:, lanes]
        out_refs[by][:, 640:768] = values_ref[:, lanes]


CHUNK = 1024
PER_CHUNK = CHUNK // BLK
PAIR = 2


def attend(q, keys, values, limit, old, total, acc):
    scores = lax.dot_general(q, keys, (((1,), (1,)), ((), ())), preferred_element_type=jnp.float32)
    tiles = [scores[:, 128 * t : 128 * (t + 1)] for t in range(keys.shape[0] // 128)]
    if limit is not None:
        tiles = [jnp.where(limit(t), a, NEGATIVE) for t, a in enumerate(tiles)]
    top = tiles[0]
    for a in tiles[1:]:
        top = jnp.maximum(top, a)
    new = jnp.maximum(old, jnp.max(top, axis=1, keepdims=True))
    shrink = jnp.exp2((old - new) * EXP2_SCALE)
    weights = [jnp.exp2((a - new) * EXP2_SCALE) for a in tiles]
    part = weights[0]
    for a in weights[1:]:
        part = part + a
    rounded = jnp.concatenate([a.astype(jnp.bfloat16) for a in weights], axis=1)
    product = jnp.dot(rounded, values, preferred_element_type=jnp.float32)
    return new, total * shrink + part, acc * shrink + product


def block_of(place_ref, i):
    return place_ref[0] * 16 + ((place_ref[1] - i // 4 + 4) % 4) * 4 + i % 4


def find_bounds(vert_ref, head, bounds):
    bounds[0] = 0
    for g in range(1, 16):
        bounds[g] = rank_of(vert_ref, head, 16 * g)
    bounds[16] = NV


def walk(place_ref, vert_ref, bounds, order, outer, at, source, kc, vc):
    y, mine1, mine2, core = (place_ref[i] for i in range(1, 5))
    head = y
    second = (mine2 - outer + 4) % 4
    for inner in range(4):
        first = (mine1 - inner + 4) % 4
        g = jnp.where(core == 0, first * 4 + second, second * 4 + first)
        start, end = bounds[g], bounds[g + 1]
        shift = at - start

        def one(entry, carry):
            block = vert_ref[head, entry]
            to = entry + shift
            order[to] = block
            if source is not None:
                slab = block // 4
                before = vert_ref[head, jnp.maximum(entry - 1, 0)] // 4
                rank = jnp.where((entry > 0) & (before == slab), BLK, 0)
                row = (inner * 4 + (y - slab % 4 + 4) % 4) * 256 + rank
                rows = pl.ds(pl.multiple_of(to * BLK, BLK), BLK)
                kc[rows, :] = source[pl.ds(pl.multiple_of(row, BLK), BLK), :]
                vc[rows, :] = source[pl.ds(pl.multiple_of(row + 128, BLK), BLK), :]
            return carry

        lax.fori_loop(start, end, one, 0)
        at = at + end - start
    return at


def chunks(place_ref, order, begin, end, ql, kc, vc, top, tot, acc):
    def one_chunk(n, carry):
        rows = pl.ds(pl.multiple_of(n * CHUNK, CHUNK), CHUNK)
        last = order[n * PER_CHUNK]
        for j in range(1, PER_CHUNK):
            last = jnp.maximum(last, order[n * PER_CHUNK + j])

        def run(masked):
            lane = lax.broadcasted_iota(jnp.int32, (1, 128), 1)

            def some(j, carry):
                for u in range(PAIR):
                    i = j * PAIR + u
                    limit = None
                    if masked:
                        mine = block_of(place_ref, i)

                        def limit(t):
                            at = n * PER_CHUNK + 2 * t
                            return jnp.where(lane < BLK, order[at], order[at + 1]) < mine

                    top[i], tot[i], acc[i] = attend(ql[i], kc[rows, :], vc[rows, :], limit, top[i], tot[i], acc[i])
                return carry

            lax.fori_loop(0, 16 // PAIR, some, 0)

        free = last < place_ref[0] * 16
        pl.when(free)(lambda: run(False))
        pl.when(jnp.logical_not(free))(lambda: run(True))
        return carry

    lax.fori_loop(begin, end, one_chunk, 0)


def near_kernel(place_ref, vert_ref, q0, q1, q2, q3, near, ql, kc, vc, top, tot, acc, bounds, order):
    for by, q in enumerate((q0, q1, q2, q3)):
        for block in range(4):
            for g in range(4):
                ql[by * 4 + block, g * BLK : (g + 1) * BLK, :] = q[block * BLK : (block + 1) * BLK, g * 128 : (g + 1) * 128]
    top[...] = jnp.full(top.shape, NEGATIVE, jnp.float32)
    tot[...] = jnp.zeros_like(tot)
    acc[...] = jnp.zeros_like(acc)
    find_bounds(vert_ref, place_ref[1], bounds)
    count = walk(place_ref, vert_ref, bounds, order, 0, jnp.int32(0), near, kc, vc)
    chunks(place_ref, order, 0, count // PER_CHUNK, ql, kc, vc, top, tot, acc)


def far_kernel(done, fresh, place_ref, vert_ref, *refs):
    sources, refs = refs[: len(fresh)], refs[len(fresh) :]
    ql, refs = refs[0], refs[6:]
    kc, vc, top, tot, acc, bounds, order = refs
    find_bounds(vert_ref, place_ref[1], bounds)
    at = jnp.int32(0)
    for outer in done:
        at = walk(place_ref, vert_ref, bounds, order, outer, at, None, kc, vc)
    begin = at // PER_CHUNK
    for outer, source in zip(fresh, sources):
        at = walk(place_ref, vert_ref, bounds, order, outer, at, source, kc, vc)
    chunks(place_ref, order, begin, at // PER_CHUNK, ql, kc, vc, top, tot, acc)


def local_kernel(place_ref, vert_ref, slash_ref, q0, q1, q2, q3, prev_ref, ql, top_in, tot_in, acc_in, top, tot, acc, kl, vl):
    group, y = place_ref[0], place_ref[1]
    head = y
    kl[0:SLAB, :] = prev_ref[:, 0:128]
    vl[0:SLAB, :] = prev_ref[:, 128:256]
    for by, q in enumerate((q0, q1, q2, q3)):
        slab = (y - by + 4) % 4
        rows = pl.ds(pl.multiple_of(SLAB + slab * SLAB, SLAB), SLAB)
        kl[rows, :] = q[:, 512:640]
        vl[rows, :] = q[:, 640:768]
    lane = lax.broadcasted_iota(jnp.int32, (256, 128), 1)
    row = lax.broadcasted_iota(jnp.int32, (256, 128), 0) % BLK

    def some(j, carry):
        for u in range(PAIR):
            i = j * PAIR + u
            block = block_of(place_ref, i)
            here = block - group * 16
            starts, valid = [here], []
            for s in range(2):
                offset = slash_ref[head, s]
                behind = block - offset
                at = jnp.minimum(rank_of(vert_ref, head, behind), NV - 1)
                ok = (behind >= 0) & (vert_ref[head, at] != behind)
                valid.append(jnp.where(ok, 256, 0))
                starts.append(here - offset)
            rows = [pl.ds(pl.multiple_of(SLAB + at * BLK, BLK), BLK) for at in starts]
            keys = jnp.concatenate([kl[r, :] for r in rows] + [kl[rows[0], :]], axis=0)
            values = jnp.concatenate([vl[r, :] for r in rows] + [vl[rows[0], :]], axis=0)

            def limit(t):
                if t == 0:
                    return lane <= jnp.where(lane < BLK, row, valid[0])
                return lane < jnp.minimum(valid[1], BLK)

            top[i], tot[i], acc[i] = attend(ql[i], keys, values, limit, top[i], tot[i], acc[i])
        return carry

    lax.fori_loop(0, 16 // PAIR, some, 0)


def finish_kernel(tot, acc, *outs):
    for by in range(4):
        for block in range(4):
            i = by * 4 + block
            o = (acc[i] / jnp.sum(tot[i], axis=1, keepdims=True)).astype(jnp.bfloat16)
            for g in range(4):
                outs[by][block * BLK : (block + 1) * BLK, g * 128 : (g + 1) * 128] = o[g * BLK : (g + 1) * BLK, :]


def project_kernel(place_ref, a0, a1, a2, a3, weight_ref, theirs_ref, mine_ref, rows_ref):
    y, core = place_ref[1], place_ref[4]

    @pl.when(pl.program_id(0) == 0)
    def _():
        for by, a in enumerate((a0, a1, a2, a3)):
            head = (y + by) % 4
            rows_ref[:, pl.ds(pl.multiple_of(head * 512, 512), 512)] = a[...]

    total = jnp.dot(rows_ref[...], weight_ref[...], preferred_element_type=jnp.float32)

    @pl.when(core == 0)
    def _():
        mine_ref[...] = total[0:128]
        theirs_ref[...] = total[128:256].astype(jnp.bfloat16)

    @pl.when(core == 1)
    def _():
        mine_ref[...] = total[128:256]
        theirs_ref[...] = total[0:128].astype(jnp.bfloat16)


SMEM = pl.BlockSpec(memory_space=pltpu.SMEM)
VMEM = pl.BlockSpec(memory_space=pltpu.VMEM)
HBM = pl.BlockSpec(memory_space=pltpu.HBM)


def bf16(*shape):
    return jax.ShapeDtypeStruct(shape, jnp.bfloat16)


def f32(*shape):
    return jax.ShapeDtypeStruct(shape, jnp.float32)


def params(limit):
    return pltpu.CompilerParams(vmem_limit_bytes=limit * MIB)


def cost(flops, moved_bytes):
    return pl.CostEstimate(flops=flops, bytes_accessed=moved_bytes, transcendentals=0)


STATE = [f32(16, 256, 128)] * 3
TABLES = [pltpu.SMEM((17,), jnp.int32), pltpu.SMEM((NV,), jnp.int32)]


def far(name, done, fresh, place, vertical, sources, ql, state, flops):
    k = len(fresh)
    return pl.pallas_call(
        functools.partial(far_kernel, done, fresh),
        out_shape=[bf16(NV * BLK, 128)] * 2 + STATE,
        in_specs=[SMEM] * 2 + [VMEM] * (k + 6),
        out_specs=[VMEM] * 5,
        scratch_shapes=TABLES,
        input_output_aliases={2 + k + 1 + n: n for n in range(5)},
        compiler_params=params(8),
        cost_estimate=cost(flops, 10**6),
        name=name,
    )(place, vertical, *sources, ql, *state)


def on_device(queries, keys, values, vertical, slash, out_weight):
    x, z, y, c = (lax.axis_index(a) for a in ALL)
    place = jnp.stack([x * 4 + z, y, jnp.where(c == 0, x, z), jnp.where(c == 0, z, x), c]).astype(jnp.int32)
    scoped = jax.named_scope
    slots = pl.pallas_call(
        slots_kernel,
        out_shape=[bf16(256, 128)] * 4,
        in_specs=[SMEM, HBM, HBM, HBM],
        out_specs=[VMEM] * 4,
        scratch_shapes=[
            pltpu.SMEM((4, NV), jnp.int32),
            pltpu.VMEM((SLAB, 512), jnp.bfloat16),
            pltpu.VMEM((SLAB, 512), jnp.bfloat16),
            pltpu.SemaphoreType.DMA((3,)),
        ],
        compiler_params=params(4),
        cost_estimate=cost(10**6, 10**6),
        name="slots",
    )(place, vertical, keys, values)
    with scoped("pick"):
        slots = [slots[0]] + [along_y(slots[by], by) for by in (1, 2, 3)]
    own = jnp.concatenate(slots, axis=0)
    split = pl.pallas_call(
        split_kernel,
        out_shape=[bf16(256, 768)] * 4,
        in_specs=[SMEM, VMEM, VMEM, VMEM],
        out_specs=[VMEM] * 4,
        compiler_params=params(8),
        cost_estimate=cost(10**6, 3 * 10**6),
        name="split",
    )(place, queries, keys, values)
    own, split = lax.optimization_barrier((own, split))
    with scoped("hop1"):
        hops = [first_hop(own, by) for by in (1, 2, 3)]
    with scoped("qkv"):
        qkv = [split[0]] + [along_y(split[by], by) for by in (1, 2, 3)]
    near = jnp.concatenate([own] + hops, axis=0)
    with scoped("hop2"):
        gathered = [second_hop(near, by) for by in (1, 3, 2)]
    last_slab = lax.select_n((y + 1) % 4, *[a[:, 512:768] for a in qkv])
    with scoped("prev"):
        prev = to_next_group(last_slab)
    ql, *state = pl.pallas_call(
        near_kernel,
        out_shape=[bf16(16, 256, 128)] + [bf16(NV * BLK, 128)] * 2 + STATE,
        in_specs=[SMEM] * 2 + [VMEM] * 5,
        out_specs=[VMEM] * 6,
        scratch_shapes=TABLES,
        compiler_params=params(8),
        cost_estimate=cost(5 * 10**9, 10**6),
        name="near",
    )(place, vertical, *qkv, near)
    state[2:] = pl.pallas_call(
        local_kernel,
        out_shape=STATE,
        in_specs=[SMEM] * 3 + [VMEM] * 9,
        out_specs=[VMEM] * 3,
        scratch_shapes=[pltpu.VMEM((5 * SLAB, 128), jnp.bfloat16)] * 2,
        input_output_aliases={9 + n: n for n in range(3)},
        compiler_params=params(8),
        cost_estimate=cost(3 * 10**9, 10**6),
        name="local",
    )(place, vertical, slash, *qkv, prev, ql, *state[2:])
    state = far("far1", (0,), (1, 3), place, vertical, gathered[:2], ql, state, 10**10)
    state = far("far2", (0, 1, 3), (2,), place, vertical, gathered[2:], ql, state, 5 * 10**9)
    attention = pl.pallas_call(
        finish_kernel,
        out_shape=[bf16(256, 512)] * 4,
        in_specs=[VMEM] * 2,
        out_specs=[VMEM] * 4,
        compiler_params=params(8),
        cost_estimate=cost(10**8, 10**6),
        name="finish",
    )(state[3], state[4])
    with scoped("back"):
        back = [attention[0]] + [along_y(attention[by], -by) for by in (1, 2, 3)]
    columns = 512
    theirs, mine = pl.pallas_call(
        project_kernel,
        grid=(4096 // columns,),
        out_shape=[bf16(128, 4096), f32(128, 4096)],
        in_specs=[SMEM] + [pl.BlockSpec((256, 512), lambda i: (0, 0))] * 4 + [pl.BlockSpec((2048, columns), lambda i: (0, i))],
        out_specs=[pl.BlockSpec((128, columns), lambda i: (0, i))] * 2,
        scratch_shapes=[pltpu.VMEM((256, 2048), jnp.bfloat16)],
        compiler_params=params(12),
        cost_estimate=cost(2 * 256 * 2048 * 4096, 2 * 10**7),
        name="project",
    )(place, *back, out_weight)
    return (mine + to_partner(theirs).astype(jnp.float32)).astype(jnp.bfloat16)


def solution(mesh):
    torus = Mesh(mesh.devices.reshape(4, 4, 4, 2), ALL)
    rows = ("x", "z", "y")
    placed = (P(rows, "c"), P(rows, "c"), P(rows, "c"), P("c", None), P("c", None), P("c", None))
    return jax.shard_map(on_device, mesh=torus, in_specs=placed, out_specs=P(ALL, None), check_vma=False)
```

```python
import functools

import jax
import jax.numpy as jnp
from jax import lax
from jax.experimental import pallas as pl
from jax.experimental.pallas import tpu as pltpu
from jax.sharding import Mesh
from jax.sharding import PartitionSpec as P

HEAD_DIM = 128
BLK = 64
SLAB = 256
NV = 64
EXP2_SCALE = HEAD_DIM ** (-0.5) * 1.4426950408889634
NEGATIVE = -1e30
ALL = ("x", "z", "y", "c")
MIB = 1 << 20


def moved(value, target):
    pairs = []
    for x in range(4):
        for z in range(4):
            for y in range(4):
                for c in range(2):
                    tx, tz, ty, tc = target(x, z, y, c)
                    pairs.append((((x * 4 + z) * 4 + y) * 2 + c, (((tx % 4) * 4 + tz % 4) * 4 + ty % 4) * 2 + tc))
    return lax.ppermute(value, ALL, pairs)


def along_y(value, by):
    return moved(value, lambda x, z, y, c: (x, z, y + by, c))


def first_hop(value, by):
    return moved(value, lambda x, z, y, c: (x + by, z, y, c) if c == 0 else (x, z + by, y, c))


def second_hop(value, by):
    return moved(value, lambda x, z, y, c: (x, z + by, y, c) if c == 0 else (x + by, z, y, c))


def to_next_group(value):
    return moved(value, lambda x, z, y, c: (x + (z + 1) // 4, z + 1, y, c))


def to_partner(value):
    return moved(value, lambda x, z, y, c: (x, z, y, 1 - c))


def rank_of(vert_ref, head, block):
    at = jnp.int32(0)
    for width in (32, 16, 8, 4, 2, 1):
        at = at + jnp.where(vert_ref[head, at + width - 1] < block, width, 0)
    return at + jnp.where(vert_ref[head, at] < block, 1, 0)


def kv_kernel(place_ref, keys_ref, values_ref, *out_refs):
    y = place_ref[1]
    for by in range(4):
        lanes = pl.ds(pl.multiple_of((y + by) % 4 * HEAD_DIM, HEAD_DIM), HEAD_DIM)
        out_refs[by][:, 0:128] = keys_ref[:, lanes]
        out_refs[by][:, 128:256] = values_ref[:, lanes]


def q_kernel(place_ref, queries_ref, *out_refs):
    y = place_ref[1]
    for by in range(4):
        out_refs[by][...] = queries_ref[:, pl.ds(pl.multiple_of((y + by) % 4 * 512, 512), 512)]


def slots_kernel(place_ref, vert_ref, kv0, kv1, kv2, kv3, own_ref, last_ref):
    group, y = place_ref[0], place_ref[1]
    for by, kv in enumerate((kv0, kv1, kv2, kv3)):
        slab = (y - by + 4) % 4
        first = (group * 4 + slab) * 4
        at = rank_of(vert_ref, y, first)
        for slot in range(2):
            entry = jnp.minimum(at + slot, NV - 1)
            block = vert_ref[y, entry] - first
            block = jnp.where((block >= 0) & (block < 4), block, 0)
            rows = pl.ds(pl.multiple_of(block * BLK, BLK), BLK)
            to = by * 256 + slot * BLK
            own_ref[to : to + BLK, :] = kv[rows, 0:128]
            own_ref[to + 128 : to + 128 + BLK, :] = kv[rows, 128:256]

        @pl.when(slab == 3)
        def _():
            last_ref[...] = kv[...]


CHUNK = 1024
PER_CHUNK = CHUNK // BLK


def scores_of(keys, q):
    return lax.dot_general(keys, q, (((1,), (1,)), ((), ())), preferred_element_type=jnp.float32)


def top_of(load, pieces):
    top = load(0)
    for t in range(1, pieces):
        top = jnp.maximum(top, load(t))
    eight = top[0:8]
    for r in range(1, 8):
        eight = jnp.maximum(eight, top[8 * r : 8 * r + 8])
    return eight


def weigh(i, load, pieces, eight, values, top, tot, acc):
    old = top[i]
    new = jnp.maximum(old, jnp.max(eight, axis=0, keepdims=True))
    level = new[0:1]
    rounded, part = [], None
    for t in range(pieces):
        weights = jnp.exp2((load(t) - level) * EXP2_SCALE)
        for r in range(8):
            piece = weights[8 * r : 8 * r + 8]
            part = piece if part is None else part + piece
        rounded.append(weights.astype(jnp.bfloat16))
    product = jnp.dot(values, jnp.concatenate(rounded, axis=0), preferred_element_type=jnp.float32)
    shrink = jnp.exp2((old - new) * EXP2_SCALE)
    top[i] = new
    tot[i] = tot[i] * shrink + part
    acc[i] = acc[i] * shrink[0:1] + product


def block_of(place_ref, i):
    return place_ref[0] * 16 + ((place_ref[1] - i // 4 + 4) % 4) * 4 + i % 4


def find_bounds(vert_ref, head, bounds):
    bounds[0] = 0
    for g in range(1, 16):
        bounds[g] = rank_of(vert_ref, head, 16 * g)
    bounds[16] = NV


def walk(place_ref, vert_ref, bounds, order, outer, at, sources, kc, vc):
    y, mine1, mine2, core = (place_ref[i] for i in range(1, 5))
    head = y
    second = (mine2 - outer + 4) % 4
    for inner in range(4):
        first = (mine1 - inner + 4) % 4
        g = jnp.where(core == 0, first * 4 + second, second * 4 + first)
        start, end = bounds[g], bounds[g + 1]
        shift = at - start

        def one(entry, carry):
            block = vert_ref[head, entry]
            to = entry + shift
            order[to] = block
            if sources is not None:
                source = sources[inner * len(sources) // 4]
                skip = inner % (4 // len(sources))
                slab = block // 4
                before = vert_ref[head, jnp.maximum(entry - 1, 0)] // 4
                rank = jnp.where((entry > 0) & (before == slab), BLK, 0)
                row = (skip * 4 + (y - slab % 4 + 4) % 4) * 256 + rank
                rows = pl.ds(pl.multiple_of(to * BLK, BLK), BLK)
                kc[rows, :] = source[pl.ds(pl.multiple_of(row, BLK), BLK), :]
                vc[rows, :] = source[pl.ds(pl.multiple_of(row + 128, BLK), BLK), :]
            return carry

        lax.fori_loop(start, end, one, 0)
        at = at + end - start
    return at


def chunks(place_ref, order, begin, end, ql, kc, vc, top, tot, acc, vt, sa, sb, ma, mb):
    def one_chunk(n, carry):
        rows = pl.ds(pl.multiple_of(n * CHUNK, CHUNK), CHUNK)
        last = order[n * PER_CHUNK]
        for j in range(1, PER_CHUNK):
            last = jnp.maximum(last, order[n * PER_CHUNK + j])
        vt[...] = vc[rows, :].T

        def score(i, buffer, eight):
            scores = scores_of(kc[rows, :], ql[i])
            buffer[...] = scores
            eight[...] = top_of(lambda t: scores[BLK * t : BLK * (t + 1)], PER_CHUNK)

        def run(masked):
            def finish(i, buffer, eight):
                def plain(t):
                    return buffer[BLK * t : BLK * (t + 1), :]

                if masked:
                    mine = block_of(place_ref, i)

                    def load(t):
                        return jnp.where(order[n * PER_CHUNK + t] < mine, plain(t), NEGATIVE)

                    weigh(i, load, PER_CHUNK, top_of(load, PER_CHUNK), vt[...], top, tot, acc)
                else:
                    weigh(i, plain, PER_CHUNK, eight[...], vt[...], top, tot, acc)

            score(0, sa, ma)
            score(1, sb, mb)

            def two(j, carry):
                finish(2 * j, sa, ma)
                score((2 * j + 2) % 16, sa, ma)
                finish(2 * j + 1, sb, mb)
                score((2 * j + 3) % 16, sb, mb)
                return carry

            lax.fori_loop(0, 8, two, 0)

        free = last < place_ref[0] * 16
        pl.when(free)(lambda: run(False))
        pl.when(jnp.logical_not(free))(lambda: run(True))
        return carry

    lax.fori_loop(begin, end, one_chunk, 0)


def part_kernel(done, fresh, splits, final, place_ref, vert_ref, *refs):
    sources, refs = list(refs[: sum(splits)]), refs[sum(splits) :]
    ql = refs[0]
    refs = refs[6:] if done else refs[4:]
    kc, vc, top, tot, acc = refs[:5]
    outs, refs = (refs[5:9], refs[9:]) if final else (None, refs[5:])
    bounds, order = refs[:2]
    find_bounds(vert_ref, place_ref[1], bounds)
    at = jnp.int32(0)
    for outer in done:
        at = walk(place_ref, vert_ref, bounds, order, outer, at, None, kc, vc)
    begin = at // PER_CHUNK
    for outer, count in zip(fresh, splits):
        at = walk(place_ref, vert_ref, bounds, order, outer, at, sources[:count], kc, vc)
        sources = sources[count:]
    chunks(place_ref, order, begin, at // PER_CHUNK, ql, kc, vc, top, tot, acc, *refs[2:])
    if final:
        for by in range(4):
            for block in range(4):
                i = by * 4 + block
                o = (acc[i] / jnp.sum(tot[i], axis=0, keepdims=True)).T.astype(jnp.bfloat16)
                for g in range(4):
                    outs[by][block * BLK : (block + 1) * BLK, g * 128 : (g + 1) * 128] = o[g * BLK : (g + 1) * BLK, :]


def local_kernel(
    place_ref, vert_ref, slash_ref, q0, q1, q2, q3, kv0, kv1, kv2, kv3, prev_ref, ql, top, tot, acc, kl, vl
):
    group, y = place_ref[0], place_ref[1]
    head = y
    kl[0:SLAB, :] = prev_ref[:, 0:128]
    vl[0:SLAB, :] = prev_ref[:, 128:256]
    for by, (q, kv) in enumerate(((q0, kv0), (q1, kv1), (q2, kv2), (q3, kv3))):
        slab = (y - by + 4) % 4
        rows = pl.ds(pl.multiple_of(SLAB + slab * SLAB, SLAB), SLAB)
        kl[rows, :] = kv[:, 0:128]
        vl[rows, :] = kv[:, 128:256]
        for block in range(4):
            for g in range(4):
                ql[by * 4 + block, g * BLK : (g + 1) * BLK, :] = q[block * BLK : (block + 1) * BLK, g * 128 : (g + 1) * 128]
    top[...] = jnp.full(top.shape, NEGATIVE, jnp.float32)
    tot[...] = jnp.zeros_like(tot)
    acc[...] = jnp.zeros_like(acc)
    key = lax.broadcasted_iota(jnp.int32, (BLK, 256), 0)
    row = lax.broadcasted_iota(jnp.int32, (BLK, 256), 1) % BLK

    def two(j, carry):
        for u in range(2):
            i = 2 * j + u
            block = block_of(place_ref, i)
            here = block - group * 16
            starts, valid = [here], []
            for s in range(2):
                offset = slash_ref[head, s]
                behind = block - offset
                at = jnp.minimum(rank_of(vert_ref, head, behind), NV - 1)
                valid.append((behind >= 0) & (vert_ref[head, at] != behind))
                starts.append(here - offset)
            rows = [pl.ds(pl.multiple_of(SLAB + at * BLK, BLK), BLK) for at in starts]
            keys = jnp.concatenate([kl[r, :] for r in rows] + [kl[rows[0], :]], axis=0)
            values = jnp.concatenate([vl[r, :] for r in rows] + [vl[rows[0], :]], axis=0).T
            scores = scores_of(keys, ql[i])

            def load(t):
                if t == 3:
                    return jnp.full((BLK, 256), NEGATIVE, jnp.float32)
                here = scores[BLK * t : BLK * (t + 1)]
                return jnp.where(key <= row if t == 0 else valid[t - 1], here, NEGATIVE)

            weigh(i, load, 4, top_of(load, 4), values, top, tot, acc)
        return carry

    lax.fori_loop(0, 8, two, 0)


def project(place_ref, a, weight_ref, by, rows, keep):
    head = (place_ref[1] + by) % 4
    depth = pl.ds(pl.multiple_of(head * 512, 512), 512)

    def tile(n, carry):
        columns = pl.ds(pl.multiple_of(n * 512, 512), 512)
        keep(columns, jnp.dot(a[rows, :], weight_ref[depth, columns], preferred_element_type=jnp.float32))
        return carry

    lax.fori_loop(0, 8, tile, 0)


def first_piece_kernel(place_ref, a, weight_ref, total_ref):
    def keep(columns, product):
        total_ref[:, columns] = product

    project(place_ref, a, weight_ref, 0, slice(None), keep)


def next_piece_kernel(by, place_ref, a, weight_ref, total_in, total_ref):
    def keep(columns, product):
        total_ref[:, columns] = total_ref[:, columns] + product

    project(place_ref, a, weight_ref, by, slice(None), keep)


def last_piece_kernel(by, mine, place_ref, a, weight_ref, total_ref, out_ref):
    core = place_ref[4]
    half = core if mine else 1 - core
    rows = pl.ds(pl.multiple_of(half * 128, 128), 128)

    def keep(columns, product):
        out_ref[:, columns] = (total_ref[rows, columns] + product).astype(out_ref.dtype)

    project(place_ref, a, weight_ref, by, rows, keep)


SMEM = pl.BlockSpec(memory_space=pltpu.SMEM)
VMEM = pl.BlockSpec(memory_space=pltpu.VMEM)


def bf16(*shape):
    return jax.ShapeDtypeStruct(shape, jnp.bfloat16)


def f32(*shape):
    return jax.ShapeDtypeStruct(shape, jnp.float32)


STATE = [f32(16, 8, 256), f32(16, 8, 256), f32(16, 128, 256)]
PACKED = [bf16(NV * BLK, 128)] * 2
WORK = [
    pltpu.SMEM((17,), jnp.int32),
    pltpu.SMEM((NV,), jnp.int32),
    pltpu.VMEM((128, CHUNK), jnp.bfloat16),
    pltpu.VMEM((CHUNK, 256), jnp.float32),
    pltpu.VMEM((CHUNK, 256), jnp.float32),
    pltpu.VMEM((8, 256), jnp.float32),
    pltpu.VMEM((8, 256), jnp.float32),
]


def call(kernel, outs, scalars, arrays, flops, limit, scratch=(), aliases=None):
    return pl.pallas_call(
        kernel,
        out_shape=outs,
        in_specs=[SMEM] * len(scalars) + [VMEM] * len(arrays),
        out_specs=[VMEM] * len(outs),
        scratch_shapes=list(scratch),
        input_output_aliases=aliases or {},
        compiler_params=pltpu.CompilerParams(vmem_limit_bytes=limit * MIB),
        cost_estimate=pl.CostEstimate(flops=int(flops), bytes_accessed=10**6, transcendentals=0),
    )(*scalars, *arrays)


def layer(queries, keys, values, vertical, slash, out_weight):
    x, z, y, c = (lax.axis_index(a) for a in ALL)
    place = jnp.stack([x * 4 + z, y, jnp.where(c == 0, x, z), jnp.where(c == 0, z, x), c]).astype(jnp.int32)
    kv = call(kv_kernel, [bf16(SLAB, 256)] * 4, [place], [keys, values], 1e6, 4)
    kv = [kv[0]] + [along_y(kv[by], by) for by in (1, 2, 3)]
    q = call(q_kernel, [bf16(SLAB, 512)] * 4, [place], [queries], 1e6, 4)
    q = [q[0]] + [along_y(q[by], by) for by in (1, 2, 3)]
    own, last = call(slots_kernel, [bf16(1024, 128), bf16(SLAB, 256)], [place, vertical], kv, 1e6, 4)
    hops = [first_hop(own, by) for by in (1, 2, 3)]
    prev = to_next_group(last)
    near = jnp.concatenate([own] + hops, axis=0)
    plus, minus = second_hop(near, 1), second_hop(near, 3)
    beyond = [second_hop(plus[:2048], 1), second_hop(minus[2048:], 3)]
    ql, *state = call(
        local_kernel, [bf16(16, 256, 128)] + STATE, [place, vertical, slash], [*q, *kv, prev], 3e9, 6,
        [pltpu.VMEM((5 * SLAB, 128), jnp.bfloat16)] * 2,
    )
    state = call(
        functools.partial(part_kernel, (), (0,), (1,), False), PACKED + STATE, [place, vertical],
        [near, ql, *state], 5e9, 8, WORK, {4 + n: 2 + n for n in range(3)},
    )
    state = call(
        functools.partial(part_kernel, (0,), (1, 3), (1, 1), False), PACKED + STATE, [place, vertical],
        [plus, minus, ql, *state], 1e10, 8, WORK, {5 + n: n for n in range(5)},
    )
    state = call(
        functools.partial(part_kernel, (0, 1, 3), (2,), (2,), True), PACKED + STATE + [bf16(SLAB, 512)] * 4,
        [place, vertical], [*beyond, ql, *state], 5e9, 8, WORK, {5 + n: n for n in range(5)},
    )
    attention = state[5:]
    back = [attention[0]] + [along_y(attention[by], -by) for by in (1, 2, 3)]
    total = call(first_piece_kernel, [f32(SLAB, 4096)], [place], [back[0], out_weight], 1e9, 6)[0]
    for by in (1, 3):
        total = call(
            functools.partial(next_piece_kernel, by), [f32(SLAB, 4096)], [place],
            [back[by], out_weight, total], 1e9, 6, (), {3: 0},
        )[0]
    theirs, mine = (
        call(
            functools.partial(last_piece_kernel, 2, own), [out], [place],
            [back[2], out_weight, total], 1e9, 6,
        )[0]
        for own, out in ((False, bf16(128, 4096)), (True, f32(128, 4096)))
    )
    other = to_partner(theirs)
    return (mine + other.astype(jnp.float32)).astype(jnp.bfloat16)


def solution(mesh):
    torus = Mesh(mesh.devices.reshape(4, 4, 4, 2), ALL)
    rows = ("x", "z", "y")
    placed = (P(rows, "c"), P(rows, "c"), P(rows, "c"), P("c", None), P("c", None), P("c", None))
    return jax.shard_map(layer, mesh=torus, in_specs=placed, out_specs=P(ALL, None), check_vma=False)
```

```python
import functools

import jax
import jax.numpy as jnp
from jax import lax
from jax.experimental import pallas as pl
from jax.experimental.pallas import tpu as pltpu
from jax.sharding import Mesh
from jax.sharding import PartitionSpec as P

HEAD_DIM = 128
BLK = 64
SLAB = 256
NV = 64
EXP2_SCALE = HEAD_DIM ** (-0.5) * 1.4426950408889634
NEGATIVE = -1e30
ALL = ("x", "z", "y", "c")
MIB = 1 << 20


def moved(value, target):
    pairs = []
    for x in range(4):
        for z in range(4):
            for y in range(4):
                for c in range(2):
                    tx, tz, ty, tc = target(x, z, y, c)
                    pairs.append((((x * 4 + z) * 4 + y) * 2 + c, (((tx % 4) * 4 + tz % 4) * 4 + ty % 4) * 2 + tc))
    return lax.ppermute(value, ALL, pairs)


def along_y(value, by):
    return moved(value, lambda x, z, y, c: (x, z, y + by, c))


def first_hop(value, by):
    return moved(value, lambda x, z, y, c: (x + by, z, y, c) if c == 0 else (x, z + by, y, c))


def second_hop(value, by):
    return moved(value, lambda x, z, y, c: (x, z + by, y, c) if c == 0 else (x + by, z, y, c))


def to_next_group(value):
    return moved(value, lambda x, z, y, c: (x + (z + 1) // 4, z + 1, y, c))


def to_partner(value):
    return moved(value, lambda x, z, y, c: (x, z, y, 1 - c))


def rank_of(vert_ref, head, block):
    at = jnp.int32(0)
    for width in (32, 16, 8, 4, 2, 1):
        at = at + jnp.where(vert_ref[head, at + width - 1] < block, width, 0)
    return at + jnp.where(vert_ref[head, at] < block, 1, 0)


def kv_kernel(place_ref, keys_ref, values_ref, *out_refs):
    y = place_ref[1]
    for by in range(4):
        lanes = pl.ds(pl.multiple_of((y + by) % 4 * HEAD_DIM, HEAD_DIM), HEAD_DIM)
        out_refs[by][:, 0:128] = keys_ref[:, lanes]
        out_refs[by][:, 128:256] = values_ref[:, lanes]


def q_kernel(place_ref, vert_ref, queries_ref, *out_refs):
    y = place_ref[1]
    for by in range(4):
        out_refs[by][...] = queries_ref[:, pl.ds(pl.multiple_of((y + by) % 4 * 512, 512), 512)]


def slots_kernel(place_ref, vert_ref, kv0, kv1, kv2, kv3, own_ref, last_ref):
    group, y = place_ref[0], place_ref[1]
    for by, kv in enumerate((kv0, kv1, kv2, kv3)):
        slab = (y - by + 4) % 4
        first = (group * 4 + slab) * 4
        at = rank_of(vert_ref, y, first)
        for slot in range(2):
            entry = jnp.minimum(at + slot, NV - 1)
            block = vert_ref[y, entry] - first
            block = jnp.where((block >= 0) & (block < 4), block, 0)
            rows = pl.ds(pl.multiple_of(block * BLK, BLK), BLK)
            to = by * 256 + slot * BLK
            own_ref[to : to + BLK, :] = kv[rows, 0:128]
            own_ref[to + 128 : to + 128 + BLK, :] = kv[rows, 128:256]

        @pl.when(slab == 3)
        def _():
            last_ref[...] = kv[...]


def join_kernel(a0, a1, a2, a3, out_ref):
    for n, a in enumerate((a0, a1, a2, a3)):
        out_ref[n * 1024 : (n + 1) * 1024, :] = a[...]


CHUNK = 1024
HALF = 512


def scores_of(keys, q):
    return lax.dot_general(keys, q, (((1,), (1,)), ((), ())), preferred_element_type=jnp.float32)


def top_of(load, pieces):
    top = load(0)
    for t in range(1, pieces):
        top = jnp.maximum(top, load(t))
    eight = top[0:8]
    for r in range(1, 8):
        eight = jnp.maximum(eight, top[8 * r : 8 * r + 8])
    return eight


def weigh(i, load, pieces, eight, values, top, tot, acc, start=False):
    new = jnp.broadcast_to(jnp.max(eight, axis=0, keepdims=True), eight.shape)
    if not start:
        old = top[i]
        new = jnp.maximum(old, new)
    level = new[0:1]
    rounded, part = [], None
    for t in range(pieces):
        weights = jnp.exp2((load(t) - level) * EXP2_SCALE)
        for r in range(8):
            piece = weights[8 * r : 8 * r + 8]
            part = piece if part is None else part + piece
        rounded.append(weights.astype(jnp.bfloat16))
    product = jnp.dot(values, jnp.concatenate(rounded, axis=0), preferred_element_type=jnp.float32)
    top[i] = new
    if start:
        tot[i] = part
        acc[i] = product
        return
    shrink = jnp.exp2((old - new) * EXP2_SCALE)
    tot[i] = tot[i] * shrink + part
    acc[i] = acc[i] * shrink[0:1] + product


def block_of(place_ref, i):
    return place_ref[0] * 16 + ((place_ref[1] - i // 4 + 4) % 4) * 4 + i % 4


def find_bounds(vert_ref, head, bounds):
    bounds[0] = 0
    for g in range(1, 16):
        bounds[g] = rank_of(vert_ref, head, 16 * g)
    bounds[16] = NV


def walk(place_ref, vert_ref, bounds, order, outer, at, sources, kc, vc):
    y, mine1, mine2, core = (place_ref[i] for i in range(1, 5))
    head = y
    second = (mine2 - outer + 4) % 4
    for inner in range(4):
        first = (mine1 - inner + 4) % 4
        g = jnp.where(core == 0, first * 4 + second, second * 4 + first)
        start, end = bounds[g], bounds[g + 1]
        shift = at - start

        def one(entry, carry):
            block = vert_ref[head, entry]
            to = entry + shift
            order[to] = block
            if sources is not None:
                source = sources[inner * len(sources) // 4]
                skip = inner % (4 // len(sources))
                slab = block // 4
                before = vert_ref[head, jnp.maximum(entry - 1, 0)] // 4
                rank = jnp.where((entry > 0) & (before == slab), BLK, 0)
                row = (skip * 4 + (y - slab % 4 + 4) % 4) * 256 + rank
                rows = pl.ds(pl.multiple_of(to * BLK, BLK), BLK)
                kc[rows, :] = source[pl.ds(pl.multiple_of(row, BLK), BLK), :]
                vc[rows, :] = source[pl.ds(pl.multiple_of(row + 128, BLK), BLK), :]
            return carry

        lax.fori_loop(start, end, one, 0)
        at = at + end - start
    return at


def chunks(size, unroll, place_ref, order, begin, count, ql, kc, vc, top, tot, acc, vt_ref, sa_ref, sb_ref, ma, mb):
    pieces = size // BLK
    vt, sa, sb = vt_ref.at[:, 0:size], sa_ref.at[0:size, :], sb_ref.at[0:size, :]

    def one_chunk(n, carry):
        first = begin + n * pieces
        rows = pl.ds(pl.multiple_of(first * BLK, HALF), size)
        last = order[first]
        for j in range(1, pieces):
            last = jnp.maximum(last, order[first + j])
        vt[...] = vc[rows, :].T

        def score(i, buffer, eight):
            scores = scores_of(kc[rows, :], ql[i])
            buffer[...] = scores
            eight[...] = top_of(lambda t: scores[BLK * t : BLK * (t + 1)], pieces)

        def run(masked):
            def finish(i, buffer, eight):
                def plain(t):
                    return buffer[BLK * t : BLK * (t + 1), :]

                if masked:
                    mine = block_of(place_ref, i)

                    def load(t):
                        return jnp.where(order[first + t] < mine, plain(t), NEGATIVE)

                    weigh(i, load, pieces, top_of(load, pieces), vt[...], top, tot, acc)
                else:
                    weigh(i, plain, pieces, eight[...], vt[...], top, tot, acc)

            score(0, sa, ma)
            score(1, sb, mb)
            each = 1 if masked else unroll

            def some(j, carry):
                for u in range(each):
                    i = 2 * (j * each + u)
                    finish(i, sa, ma)
                    score((i + 2) % 16, sa, ma)
                    finish(i + 1, sb, mb)
                    score((i + 3) % 16, sb, mb)
                return carry

            lax.fori_loop(0, 8 // each, some, 0)

        free = last < place_ref[0] * 16
        pl.when(free)(lambda: run(False))
        pl.when(jnp.logical_not(free))(lambda: run(True))
        return carry

    lax.fori_loop(0, count, one_chunk, 0)


def part_kernel(stage, place_ref, vert_ref, *refs):
    splits = ((1,), (1, 1), (2,))[stage]
    sources, refs = refs[: sum(splits)], refs[sum(splits) :]
    ql = refs[0]
    refs = refs[6:] if stage else refs[4:]
    final = stage == 2
    outs = refs[5:9] if final else None
    bounds, order = refs[9:11] if final else refs[5:7]
    work = (ql, *refs[:5], *(refs[11:] if final else refs[7:]))
    kc, vc, _, tot, acc = refs[:5]
    find_bounds(vert_ref, place_ref[1], bounds)

    def add(outer, at, fresh):
        return walk(place_ref, vert_ref, bounds, order, outer, at, fresh, kc, vc)

    near = add(0, jnp.int32(0), sources if stage == 0 else None)
    begin = near // 8 * 8
    if stage == 0:
        chunks(HALF, 2, place_ref, order, jnp.int32(0), near // 8, *work)
    else:
        at = add(1, near, sources[:1] if stage == 1 else None)
        at = add(3, at, sources[1:] if stage == 1 else None)
        whole = (at - begin) // 16
        if stage == 1:
            chunks(CHUNK, 2, place_ref, order, begin, whole, *work)
        else:
            add(2, at, sources)
            begin = begin + whole * 16
            left = (NV - begin) // 16
            chunks(CHUNK, 2, place_ref, order, begin, left, *work)
            begin = begin + left * 16
            chunks(HALF, 1, place_ref, order, begin, (NV - begin) // 8, *work)
    if final:
        for by in range(4):
            for block in range(4):
                i = by * 4 + block
                o = (acc[i] / jnp.sum(tot[i], axis=0, keepdims=True)).T.astype(jnp.bfloat16)
                for g in range(4):
                    outs[by][block * BLK : (block + 1) * BLK, g * 128 : (g + 1) * 128] = o[g * BLK : (g + 1) * BLK, :]


def local_kernel(
    place_ref, vert_ref, slash_ref, q0, q1, q2, q3, kv0, kv1, kv2, kv3, prev_ref, ql, top, tot, acc, kl, vl
):
    group, y = place_ref[0], place_ref[1]
    head = y
    kl[0:SLAB, :] = prev_ref[:, 0:128]
    vl[0:SLAB, :] = prev_ref[:, 128:256]
    for by, (q, kv) in enumerate(((q0, kv0), (q1, kv1), (q2, kv2), (q3, kv3))):
        slab = (y - by + 4) % 4
        rows = pl.ds(pl.multiple_of(SLAB + slab * SLAB, SLAB), SLAB)
        kl[rows, :] = kv[:, 0:128]
        vl[rows, :] = kv[:, 128:256]
        for block in range(4):
            for g in range(4):
                ql[by * 4 + block, g * BLK : (g + 1) * BLK, :] = q[block * BLK : (block + 1) * BLK, g * 128 : (g + 1) * 128]
    key = lax.broadcasted_iota(jnp.int32, (BLK, 256), 0)
    row = lax.broadcasted_iota(jnp.int32, (BLK, 256), 1) % BLK

    def some(j, carry):
        for u in range(4):
            i = 4 * j + u
            block = block_of(place_ref, i)
            here = block - group * 16
            starts, valid = [here], []
            for s in range(2):
                offset = slash_ref[head, s]
                behind = block - offset
                at = jnp.minimum(rank_of(vert_ref, head, behind), NV - 1)
                valid.append((behind >= 0) & (vert_ref[head, at] != behind))
                starts.append(here - offset)
            rows = [pl.ds(pl.multiple_of(SLAB + at * BLK, BLK), BLK) for at in starts]
            keys = jnp.concatenate([kl[r, :] for r in rows] + [kl[rows[0], :]], axis=0)
            values = jnp.concatenate([vl[r, :] for r in rows] + [vl[rows[0], :]], axis=0).T
            scores = scores_of(keys, ql[i])

            def load(t):
                if t == 3:
                    return jnp.full((BLK, 256), NEGATIVE, jnp.float32)
                here = scores[BLK * t : BLK * (t + 1)]
                return jnp.where(key <= row if t == 0 else valid[t - 1], here, NEGATIVE)

            weigh(i, load, 4, top_of(load, 4), values, top, tot, acc, True)
        return carry

    lax.fori_loop(0, 4, some, 0)


def project(place_ref, a, weight_ref, by, rows, keep):
    head = (place_ref[1] + by) % 4
    depth = pl.ds(pl.multiple_of(head * 512, 512), 512)

    for n in range(8):
        columns = slice(n * 512, (n + 1) * 512)
        keep(columns, jnp.dot(a[rows, :], weight_ref[depth, columns], preferred_element_type=jnp.float32))


def first_piece_kernel(place_ref, a, weight_ref, total_ref):
    def keep(columns, product):
        total_ref[:, columns] = product

    project(place_ref, a, weight_ref, 0, slice(None), keep)


def next_piece_kernel(by, place_ref, a, weight_ref, total_in, total_ref):
    def keep(columns, product):
        total_ref[:, columns] = total_ref[:, columns] + product

    project(place_ref, a, weight_ref, by, slice(None), keep)


def last_piece_kernel(by, mine, place_ref, a, weight_ref, total_ref, out_ref):
    core = place_ref[4]
    half = core if mine else 1 - core
    rows = pl.ds(pl.multiple_of(half * 128, 128), 128)

    def keep(columns, product):
        out_ref[:, columns] = (total_ref[rows, columns] + product).astype(out_ref.dtype)

    project(place_ref, a, weight_ref, by, rows, keep)


SMEM = pl.BlockSpec(memory_space=pltpu.SMEM)
VMEM = pl.BlockSpec(memory_space=pltpu.VMEM)


def bf16(*shape):
    return jax.ShapeDtypeStruct(shape, jnp.bfloat16)


def f32(*shape):
    return jax.ShapeDtypeStruct(shape, jnp.float32)


STATE = [f32(16, 8, 256), f32(16, 8, 256), f32(16, 128, 256)]
PACKED = [bf16(NV * BLK, 128)] * 2
WORK = [
    pltpu.SMEM((17,), jnp.int32),
    pltpu.SMEM((NV,), jnp.int32),
    pltpu.VMEM((128, CHUNK), jnp.bfloat16),
    pltpu.VMEM((CHUNK, 256), jnp.float32),
    pltpu.VMEM((CHUNK, 256), jnp.float32),
    pltpu.VMEM((8, 256), jnp.float32),
    pltpu.VMEM((8, 256), jnp.float32),
]


def call(kernel, outs, scalars, arrays, flops, limit, scratch=(), aliases=None):
    return pl.pallas_call(
        kernel,
        out_shape=outs,
        in_specs=[SMEM] * len(scalars) + [VMEM] * len(arrays),
        out_specs=[VMEM] * len(outs),
        scratch_shapes=list(scratch),
        input_output_aliases=aliases or {},
        compiler_params=pltpu.CompilerParams(vmem_limit_bytes=limit * MIB),
        cost_estimate=pl.CostEstimate(flops=int(flops), bytes_accessed=10**6, transcendentals=0),
    )(*scalars, *arrays)


def layer(queries, keys, values, vertical, slash, out_weight):
    x, z, y, c = (lax.axis_index(a) for a in ALL)
    place = jnp.stack([x * 4 + z, y, jnp.where(c == 0, x, z), jnp.where(c == 0, z, x), c]).astype(jnp.int32)
    kv = call(kv_kernel, [bf16(SLAB, 256)] * 4, [place], [keys, values], 1e6, 4)
    kv = [kv[0]] + [along_y(kv[by], by) for by in (1, 2, 3)]
    q = call(q_kernel, [bf16(SLAB, 512)] * 4, [place, vertical], [queries], 1e6, 4)
    q = [q[0]] + [along_y(q[by], by) for by in (1, 2, 3)]
    own, last = call(slots_kernel, [bf16(1024, 128), bf16(SLAB, 256)], [place, vertical], kv, 1e6, 4)
    hops = [first_hop(own, by) for by in (1, 2, 3)]
    prev = to_next_group(last)
    near = call(join_kernel, [bf16(4096, 128)], [], [own, *hops], 1e6, 4)[0]
    plus, minus = second_hop(near, 1), second_hop(near, 3)
    beyond = [second_hop(plus[:2048], 1), second_hop(minus[2048:], 3)]
    ql, *state = call(
        local_kernel, [bf16(16, 256, 128)] + STATE, [place, vertical, slash], [*q, *kv, prev], 3e9, 6,
        [pltpu.VMEM((5 * SLAB, 128), jnp.bfloat16)] * 2,
    )
    state = call(
        functools.partial(part_kernel, 0), PACKED + STATE, [place, vertical],
        [near, ql, *state], 5e9, 8, WORK, {4 + n: 2 + n for n in range(3)},
    )
    state = call(
        functools.partial(part_kernel, 1), PACKED + STATE, [place, vertical],
        [plus, minus, ql, *state], 1e10, 8, WORK, {5 + n: n for n in range(5)},
    )
    state = call(
        functools.partial(part_kernel, 2), PACKED + STATE + [bf16(SLAB, 512)] * 4,
        [place, vertical], [*beyond, ql, *state], 5e9, 8, WORK, {5 + n: n for n in range(5)},
    )
    attention = state[5:]
    back = [attention[0]] + [along_y(attention[by], -by) for by in (1, 2, 3)]
    total = call(first_piece_kernel, [f32(SLAB, 4096)], [place], [back[0], out_weight], 1e9, 6)[0]
    for by in (1, 3):
        total = call(
            functools.partial(next_piece_kernel, by), [f32(SLAB, 4096)], [place],
            [back[by], out_weight, total], 1e9, 6, (), {3: 0},
        )[0]
    theirs, mine = (
        call(
            functools.partial(last_piece_kernel, 2, own), [out], [place],
            [back[2], out_weight, total], 1e9, 6,
        )[0]
        for own, out in ((False, bf16(128, 4096)), (True, f32(128, 4096)))
    )
    other = to_partner(theirs)
    return (mine + other.astype(jnp.float32)).astype(jnp.bfloat16)


def solution(mesh):
    torus = Mesh(mesh.devices.reshape(4, 4, 4, 2), ALL)
    rows = ("x", "z", "y")
    placed = (P(rows, "c"), P(rows, "c"), P(rows, "c"), P("c", None), P("c", None), P("c", None))
    return jax.shard_map(layer, mesh=torus, in_specs=placed, out_specs=P(ALL, None), check_vma=False)
```

```python
import functools

import jax
import jax.numpy as jnp
from jax import lax
from jax.experimental import pallas as pl
from jax.experimental.pallas import tpu as pltpu
from jax.sharding import Mesh
from jax.sharding import PartitionSpec as P

HEAD_DIM = 128
BLK = 64
SLAB = 256
NV = 64
EXP2_SCALE = HEAD_DIM ** (-0.5) * 1.4426950408889634
NEGATIVE = -1e30
SLASH = 8
VERT = 16
NEVER = 1 << 20
ALL = ("x", "z", "y", "c")
MIB = 1 << 20


def moved(value, target):
    pairs = []
    for x in range(4):
        for z in range(4):
            for y in range(4):
                for c in range(2):
                    tx, tz, ty, tc = target(x, z, y, c)
                    pairs.append((((x * 4 + z) * 4 + y) * 2 + c, (((tx % 4) * 4 + tz % 4) * 4 + ty % 4) * 2 + tc))
    return lax.ppermute(value, ALL, pairs)


def along_y(value, by):
    return moved(value, lambda x, z, y, c: (x, z, y + by, c))


def first_hop(value, by):
    return moved(value, lambda x, z, y, c: (x + by, z, y, c) if c == 0 else (x, z + by, y, c))


def second_hop(value, by):
    return moved(value, lambda x, z, y, c: (x, z + by, y, c) if c == 0 else (x + by, z, y, c))


def to_next_group(value):
    return moved(value, lambda x, z, y, c: (x + (z + 1) // 4, z + 1, y, c))


def to_partner(value):
    return moved(value, lambda x, z, y, c: (x, z, y, 1 - c))


def row_rank(table_ref, block):
    at = jnp.int32(VERT)
    for width in (32, 16, 8, 4, 2, 1):
        at = at + jnp.where(table_ref[at + width - 1] < block, width, 0)
    return at - VERT + jnp.where(table_ref[at] < block, 1, 0)


def kv_kernel(place_ref, keys_ref, values_ref, *out_refs):
    y = place_ref[1]
    for by in range(4):
        lanes = pl.ds(pl.multiple_of((y + by) % 4 * HEAD_DIM, HEAD_DIM), HEAD_DIM)
        out_refs[by][:, 0:128] = keys_ref[:, lanes]
        out_refs[by][:, 128:256] = values_ref[:, lanes]


def q_kernel(place_ref, queries_ref, *out_refs):
    y = place_ref[1]
    for by in range(4):
        out_refs[by][...] = queries_ref[:, pl.ds(pl.multiple_of((y + by) % 4 * 512, 512), 512)]


def slots_kernel(place_ref, vert_ref, slash_ref, kv0, kv1, kv2, kv3, own_ref, last_ref, table_ref):
    group, y = place_ref[0], place_ref[1]
    for n in range(5):
        table_ref[n] = place_ref[n]
    for n in range(2):
        table_ref[SLASH + n] = slash_ref[y, n]
    for n in range(NV):
        table_ref[VERT + n] = vert_ref[y, n]
    for by, kv in enumerate((kv0, kv1, kv2, kv3)):
        slab = (y - by + 4) % 4
        first = (group * 4 + slab) * 4
        at = row_rank(table_ref, first)
        for slot in range(2):
            entry = jnp.minimum(at + slot, NV - 1)
            block = table_ref[VERT + entry] - first
            block = jnp.where((block >= 0) & (block < 4), block, 0)
            rows = pl.ds(pl.multiple_of(block * BLK, BLK), BLK)
            to = by * 256 + slot * BLK
            own_ref[to : to + BLK, :] = kv[rows, 0:128]
            own_ref[to + 128 : to + 128 + BLK, :] = kv[rows, 128:256]

        @pl.when(slab == 3)
        def _():
            last_ref[...] = kv[...]


def join_kernel(a0, a1, a2, a3, out_ref):
    for n, a in enumerate((a0, a1, a2, a3)):
        out_ref[n * 1024 : (n + 1) * 1024, :] = a[...]


CHUNK = 1024
HALF = 512


def scores_of(keys, q):
    return lax.dot_general(keys, q, (((1,), (1,)), ((), ())), preferred_element_type=jnp.float32)


def top_of(load, pieces):
    top = load(0)
    for t in range(1, pieces):
        top = jnp.maximum(top, load(t))
    eight = top[0:8]
    for r in range(1, 8):
        eight = jnp.maximum(eight, top[8 * r : 8 * r + 8])
    return eight


def weigh(i, load, pieces, eight, values, top, tot, acc, start=False):
    new = jnp.broadcast_to(jnp.max(eight, axis=0, keepdims=True), eight.shape)
    if not start:
        old = top[i]
        new = jnp.maximum(old, new)
    level = new[0:1]
    rounded, part = [], None
    for t in range(pieces):
        weights = jnp.exp2((load(t) - level) * EXP2_SCALE)
        for r in range(8):
            piece = weights[8 * r : 8 * r + 8]
            part = piece if part is None else part + piece
        rounded.append(weights.astype(jnp.bfloat16))
    product = jnp.dot(values, jnp.concatenate(rounded, axis=0), preferred_element_type=jnp.float32)
    top[i] = new
    if start:
        tot[i] = part
        acc[i] = product
        return
    shrink = jnp.exp2((old - new) * EXP2_SCALE)
    tot[i] = tot[i] * shrink + part
    acc[i] = acc[i] * shrink[0:1] + product


def block_of(place_ref, i):
    return place_ref[0] * 16 + ((place_ref[1] - i // 4 + 4) % 4) * 4 + i % 4


def find_bounds(place_ref, bounds):
    bounds[0] = 0
    for g in range(1, 16):
        bounds[g] = row_rank(place_ref, 16 * g)
    bounds[16] = NV


def walk(place_ref, bounds, order, outer, at, sources, kc, vc):
    group, y, mine1, mine2, core = (place_ref[i] for i in range(5))
    second = (mine2 - outer + 4) % 4
    for inner in range(4):
        first = (mine1 - inner + 4) % 4
        g = jnp.where(core == 0, first * 4 + second, second * 4 + first)
        start = bounds[g]
        end = jnp.where(g <= group, bounds[g + 1], start)
        shift = at - start

        def one(entry, carry):
            block = place_ref[VERT + entry]
            to = entry + shift
            order[to] = block
            if sources is not None:
                source = sources[inner * len(sources) // 4]
                skip = inner % (4 // len(sources))
                slab = block // 4
                before = place_ref[VERT + jnp.maximum(entry - 1, 0)] // 4
                rank = jnp.where((entry > 0) & (before == slab), BLK, 0)
                row = (skip * 4 + (y - slab % 4 + 4) % 4) * 256 + rank
                rows = pl.ds(pl.multiple_of(to * BLK, BLK), BLK)
                kc[rows, :] = source[pl.ds(pl.multiple_of(row, BLK), BLK), :]
                vc[rows, :] = source[pl.ds(pl.multiple_of(row + 128, BLK), BLK), :]
            return carry

        lax.fori_loop(start, end, one, 0)
        at = at + end - start
    return at


def chunks(size, unroll, place_ref, order, begin, count, ql, kc, vc, top, tot, acc, vt_ref, sa_ref, sb_ref, ma, mb):
    pieces = size // BLK
    vt, sa, sb = vt_ref.at[:, 0:size], sa_ref.at[0:size, :], sb_ref.at[0:size, :]

    def one_chunk(n, carry):
        first = begin + n * pieces
        rows = pl.ds(pl.multiple_of(first * BLK, HALF), size)
        last = order[first]
        for j in range(1, pieces):
            last = jnp.maximum(last, order[first + j])
        vt[...] = vc[rows, :].T

        def score(i, buffer, eight):
            scores = scores_of(kc[rows, :], ql[i])
            buffer[...] = scores
            eight[...] = top_of(lambda t: scores[BLK * t : BLK * (t + 1)], pieces)

        def run(masked):
            def finish(i, buffer, eight):
                def plain(t):
                    return buffer[BLK * t : BLK * (t + 1), :]

                if masked:
                    mine = block_of(place_ref, i)

                    def load(t):
                        return jnp.where(order[first + t] < mine, plain(t), NEGATIVE)

                    weigh(i, load, pieces, top_of(load, pieces), vt[...], top, tot, acc)
                else:
                    weigh(i, plain, pieces, eight[...], vt[...], top, tot, acc)

            score(0, sa, ma)
            score(1, sb, mb)
            each = 1 if masked else unroll

            def some(j, carry):
                for u in range(each):
                    i = 2 * (j * each + u)
                    finish(i, sa, ma)
                    score((i + 2) % 16, sa, ma)
                    finish(i + 1, sb, mb)
                    score((i + 3) % 16, sb, mb)
                return carry

            lax.fori_loop(0, 8 // each, some, 0)

        free = last < place_ref[0] * 16
        pl.when(free)(lambda: run(False))
        pl.when(jnp.logical_not(free))(lambda: run(True))
        return carry

    lax.fori_loop(0, count, one_chunk, 0)


def part_kernel(stage, place_ref, *refs):
    splits = ((1,), (1, 1), (2,))[stage]
    sources, refs = refs[: sum(splits)], refs[sum(splits) :]
    ql = refs[0]
    refs = refs[6:] if stage else refs[4:]
    final = stage == 2
    outs = refs[5:9] if final else None
    bounds, order = refs[9:11] if final else refs[5:7]
    work = (ql, *refs[:5], *(refs[11:] if final else refs[7:]))
    kc, vc, _, tot, acc = refs[:5]
    find_bounds(place_ref, bounds)

    def add(outer, at, fresh):
        return walk(place_ref, bounds, order, outer, at, fresh, kc, vc)

    near = add(0, jnp.int32(0), sources if stage == 0 else None)
    begin = near // 8 * 8
    if stage == 0:
        chunks(HALF, 2, place_ref, order, jnp.int32(0), near // 8, *work)
    else:
        at = add(1, near, sources[:1] if stage == 1 else None)
        at = add(3, at, sources[1:] if stage == 1 else None)
        whole = (at - begin) // 16
        if stage == 1:
            chunks(CHUNK, 2, place_ref, order, begin, whole, *work)
        else:
            at = add(2, at, sources)
            begin = begin + whole * 16
            left = (at - begin) // 16
            chunks(CHUNK, 2, place_ref, order, begin, left, *work)
            begin = begin + left * 16
            left = (at - begin + 7) // 8

            def clear(n, carry):
                order[n] = NEVER
                vc[pl.ds(pl.multiple_of(n * BLK, BLK), BLK), :] = jnp.zeros((BLK, 128), jnp.bfloat16)
                return carry

            lax.fori_loop(at, begin + left * 8, clear, 0)
            chunks(HALF, 1, place_ref, order, begin, left, *work)
    if final:
        for by in range(4):
            for block in range(4):
                i = by * 4 + block
                o = (acc[i] / jnp.sum(tot[i], axis=0, keepdims=True)).T.astype(jnp.bfloat16)
                for g in range(4):
                    outs[by][block * BLK : (block + 1) * BLK, g * 128 : (g + 1) * 128] = o[g * BLK : (g + 1) * BLK, :]


def local_kernel(
    place_ref, q0, q1, q2, q3, kv0, kv1, kv2, kv3, prev_ref, ql, top, tot, acc, kl, vl
):
    group, y = place_ref[0], place_ref[1]
    kl[0:SLAB, :] = prev_ref[:, 0:128]
    vl[0:SLAB, :] = prev_ref[:, 128:256]
    for by, (q, kv) in enumerate(((q0, kv0), (q1, kv1), (q2, kv2), (q3, kv3))):
        slab = (y - by + 4) % 4
        rows = pl.ds(pl.multiple_of(SLAB + slab * SLAB, SLAB), SLAB)
        kl[rows, :] = kv[:, 0:128]
        vl[rows, :] = kv[:, 128:256]
        for block in range(4):
            for g in range(4):
                ql[by * 4 + block, g * BLK : (g + 1) * BLK, :] = q[block * BLK : (block + 1) * BLK, g * 128 : (g + 1) * 128]
    key = lax.broadcasted_iota(jnp.int32, (BLK, 256), 0)
    row = lax.broadcasted_iota(jnp.int32, (BLK, 256), 1) % BLK

    def some(j, carry):
        ready = []
        for u in range(4):
            i = 4 * j + u
            block = block_of(place_ref, i)
            here = block - group * 16
            starts, valid = [here], []
            for s in range(2):
                offset = place_ref[SLASH + s]
                behind = block - offset
                at = jnp.minimum(row_rank(place_ref, behind), NV - 1)
                valid.append((behind >= 0) & (place_ref[VERT + at] != behind))
                starts.append(here - offset)
            rows = [pl.ds(pl.multiple_of(SLAB + at * BLK, BLK), BLK) for at in starts]
            keys = jnp.concatenate([kl[r, :] for r in rows] + [kl[rows[0], :]], axis=0)
            values = jnp.concatenate([vl[r, :] for r in rows] + [vl[rows[0], :]], axis=0).T
            ready.append((i, scores_of(keys, ql[i]), values, valid))
        for i, scores, values, valid in ready:
            def load(t):
                if t == 3:
                    return jnp.full((BLK, 256), NEGATIVE, jnp.float32)
                here = scores[BLK * t : BLK * (t + 1)]
                return jnp.where(key <= row if t == 0 else valid[t - 1], here, NEGATIVE)

            weigh(i, load, 4, top_of(load, 4), values, top, tot, acc, True)
        return carry

    lax.fori_loop(0, 4, some, 0)


def project(place_ref, a, weight_ref, by, rows, keep):
    head = (place_ref[1] + by) % 4
    depth = pl.ds(pl.multiple_of(head * 512, 512), 512)

    for n in range(8):
        columns = slice(n * 512, (n + 1) * 512)
        keep(columns, jnp.dot(a[rows, :], weight_ref[depth, columns], preferred_element_type=jnp.float32))


def first_piece_kernel(place_ref, a, weight_ref, total_ref):
    def keep(columns, product):
        total_ref[:, columns] = product

    project(place_ref, a, weight_ref, 0, slice(None), keep)


def next_piece_kernel(by, place_ref, a, weight_ref, total_in, total_ref):
    def keep(columns, product):
        total_ref[:, columns] = total_ref[:, columns] + product

    project(place_ref, a, weight_ref, by, slice(None), keep)


def last_piece_kernel(by, mine, place_ref, a, weight_ref, total_ref, out_ref):
    core = place_ref[4]
    half = core if mine else 1 - core
    rows = pl.ds(pl.multiple_of(half * 128, 128), 128)

    def keep(columns, product):
        out_ref[:, columns] = (total_ref[rows, columns] + product).astype(out_ref.dtype)

    project(place_ref, a, weight_ref, by, rows, keep)


SMEM = pl.BlockSpec(memory_space=pltpu.SMEM)
VMEM = pl.BlockSpec(memory_space=pltpu.VMEM)


def bf16(*shape):
    return jax.ShapeDtypeStruct(shape, jnp.bfloat16)


def f32(*shape):
    return jax.ShapeDtypeStruct(shape, jnp.float32)


STATE = [f32(16, 8, 256), f32(16, 8, 256), f32(16, 128, 256)]
PACKED = [bf16(NV * BLK, 128)] * 2
WORK = [
    pltpu.SMEM((17,), jnp.int32),
    pltpu.SMEM((NV,), jnp.int32),
    pltpu.VMEM((128, CHUNK), jnp.bfloat16),
    pltpu.VMEM((CHUNK, 256), jnp.float32),
    pltpu.VMEM((CHUNK, 256), jnp.float32),
    pltpu.VMEM((8, 256), jnp.float32),
    pltpu.VMEM((8, 256), jnp.float32),
]


def call(kernel, outs, scalars, arrays, flops, limit, scratch=(), aliases=None):
    return pl.pallas_call(
        kernel,
        out_shape=outs,
        in_specs=[SMEM] * len(scalars) + [VMEM] * len(arrays),
        out_specs=[VMEM] * len(outs),
        scratch_shapes=list(scratch),
        input_output_aliases=aliases or {},
        compiler_params=pltpu.CompilerParams(vmem_limit_bytes=limit * MIB),
        cost_estimate=pl.CostEstimate(flops=int(flops), bytes_accessed=10**6, transcendentals=0),
    )(*scalars, *arrays)


def layer(queries, keys, values, vertical, slash, out_weight):
    x, z, y, c = (lax.axis_index(a) for a in ALL)
    place = jnp.stack([x * 4 + z, y, jnp.where(c == 0, x, z), jnp.where(c == 0, z, x), c]).astype(jnp.int32)
    kv = call(kv_kernel, [bf16(SLAB, 256)] * 4, [place], [keys, values], 1e6, 4)
    kv = [kv[0]] + [along_y(kv[by], by) for by in (1, 2, 3)]
    q = call(q_kernel, [bf16(SLAB, 512)] * 4, [place], [queries], 1e6, 4)
    q = [q[0]] + [along_y(q[by], by) for by in (1, 2, 3)]
    own, last, table = pl.pallas_call(
        slots_kernel,
        out_shape=[bf16(1024, 128), bf16(SLAB, 256), jax.ShapeDtypeStruct((128,), jnp.int32)],
        in_specs=[SMEM] * 3 + [VMEM] * 4,
        out_specs=[VMEM, VMEM, SMEM],
        compiler_params=pltpu.CompilerParams(vmem_limit_bytes=4 * MIB),
        cost_estimate=pl.CostEstimate(flops=10**6, bytes_accessed=10**6, transcendentals=0),
        name="slots",
    )(place, vertical, slash, *kv)
    hops = [first_hop(own, by) for by in (1, 2, 3)]
    prev = to_next_group(last)
    near = call(join_kernel, [bf16(4096, 128)], [], [own, *hops], 1e6, 4)[0]
    plus, minus = second_hop(near, 1), second_hop(near, 3)
    beyond = [second_hop(plus[:2048], 1), second_hop(minus[2048:], 3)]
    ql, *state = call(
        local_kernel, [bf16(16, 256, 128)] + STATE, [table], [*q, *kv, prev], 3e9, 6,
        [pltpu.VMEM((5 * SLAB, 128), jnp.bfloat16)] * 2,
    )
    state = call(
        functools.partial(part_kernel, 0), PACKED + STATE, [table],
        [near, ql, *state], 5e9, 8, WORK, {3 + n: 2 + n for n in range(3)},
    )
    state = call(
        functools.partial(part_kernel, 1), PACKED + STATE, [table],
        [plus, minus, ql, *state], 1e10, 8, WORK, {4 + n: n for n in range(5)},
    )
    state = call(
        functools.partial(part_kernel, 2), PACKED + STATE + [bf16(SLAB, 512)] * 4,
        [table], [*beyond, ql, *state], 5e9, 8, WORK, {4 + n: n for n in range(5)},
    )
    attention = state[5:]
    back = [attention[0]] + [along_y(attention[by], -by) for by in (1, 2, 3)]
    total = call(first_piece_kernel, [f32(SLAB, 4096)], [place], [back[0], out_weight], 1e9, 6)[0]
    for by in (1, 3):
        total = call(
            functools.partial(next_piece_kernel, by), [f32(SLAB, 4096)], [place],
            [back[by], out_weight, total], 1e9, 6, (), {3: 0},
        )[0]
    theirs, mine = (
        call(
            functools.partial(last_piece_kernel, 2, own), [out], [place],
            [back[2], out_weight, total], 1e9, 6,
        )[0]
        for own, out in ((False, bf16(128, 4096)), (True, f32(128, 4096)))
    )
    other = to_partner(theirs)
    return (mine + other.astype(jnp.float32)).astype(jnp.bfloat16)


def solution(mesh):
    torus = Mesh(mesh.devices.reshape(4, 4, 4, 2), ALL)
    rows = ("x", "z", "y")
    placed = (P(rows, "c"), P(rows, "c"), P(rows, "c"), P("c", None), P("c", None), P("c", None))
    return jax.shard_map(layer, mesh=torus, in_specs=placed, out_specs=P(ALL, None), check_vma=False)
```

```python
import functools

import jax
import jax.numpy as jnp
from jax import lax
from jax.experimental import pallas as pl
from jax.experimental.pallas import tpu as pltpu
from jax.sharding import Mesh
from jax.sharding import PartitionSpec as P

HEAD_DIM = 128
BLK = 64
SLAB = 256
NV = 64
EXP2_SCALE = HEAD_DIM ** (-0.5) * 1.4426950408889634
NEGATIVE = -1e30
SLASH = 8
VERT = 16
NEVER = 1 << 20
ALL = ("x", "z", "y", "c")
MIB = 1 << 20


def moved(value, target):
    pairs = []
    for x in range(4):
        for z in range(4):
            for y in range(4):
                for c in range(2):
                    tx, tz, ty, tc = target(x, z, y, c)
                    pairs.append((((x * 4 + z) * 4 + y) * 2 + c, (((tx % 4) * 4 + tz % 4) * 4 + ty % 4) * 2 + tc))
    return lax.ppermute(value, ALL, pairs)


def along_y(value, by):
    return moved(value, lambda x, z, y, c: (x, z, y + by, c))


def first_hop(value, by):
    return moved(value, lambda x, z, y, c: (x + by, z, y, c) if c == 0 else (x, z + by, y, c))


def second_hop(value, by):
    return moved(value, lambda x, z, y, c: (x, z + by, y, c) if c == 0 else (x + by, z, y, c))


def to_next_group(value):
    return moved(value, lambda x, z, y, c: (x + (z + 1) // 4, z + 1, y, c))


def to_partner(value):
    return moved(value, lambda x, z, y, c: (x, z, y, 1 - c))


def row_rank(table_ref, block):
    at = jnp.int32(VERT)
    for width in (32, 16, 8, 4, 2, 1):
        at = at + jnp.where(table_ref[at + width - 1] < block, width, 0)
    return at - VERT + jnp.where(table_ref[at] < block, 1, 0)


def kv_kernel(place_ref, keys_ref, values_ref, *out_refs):
    y = place_ref[1]
    for by in range(4):
        lanes = pl.ds(pl.multiple_of((y + by) % 4 * HEAD_DIM, HEAD_DIM), HEAD_DIM)
        out_refs[by][:, 0:128] = keys_ref[:, lanes]
        out_refs[by][:, 128:256] = values_ref[:, lanes]


def q_kernel(place_ref, queries_ref, *out_refs):
    y = place_ref[1]
    for by in range(4):
        out_refs[by][...] = queries_ref[:, pl.ds(pl.multiple_of((y + by) % 4 * 512, 512), 512)]


def slots_kernel(place_ref, vert_ref, slash_ref, kv0, kv1, kv2, kv3, own_ref, last_ref, table_ref):
    group, y = place_ref[0], place_ref[1]
    for n in range(5):
        table_ref[n] = place_ref[n]
    for n in range(2):
        table_ref[SLASH + n] = slash_ref[n, y]
    for n in range(NV):
        table_ref[VERT + n] = vert_ref[y, n]
    for by, kv in enumerate((kv0, kv1, kv2, kv3)):
        slab = (y - by + 4) % 4
        first = (group * 4 + slab) * 4
        at = row_rank(table_ref, first)
        for slot in range(2):
            entry = jnp.minimum(at + slot, NV - 1)
            block = table_ref[VERT + entry] - first
            block = jnp.where((block >= 0) & (block < 4), block, 0)
            rows = pl.ds(pl.multiple_of(block * BLK, BLK), BLK)
            to = by * 256 + slot * BLK
            own_ref[to : to + BLK, :] = kv[rows, 0:128]
            own_ref[to + 128 : to + 128 + BLK, :] = kv[rows, 128:256]

        @pl.when(slab == 3)
        def _():
            last_ref[...] = kv[...]


def join_kernel(a0, a1, a2, a3, out_ref):
    for n, a in enumerate((a0, a1, a2, a3)):
        out_ref[n * 1024 : (n + 1) * 1024, :] = a[...]


CHUNK = 1024
HALF = 512
EVERY = (0, 1, 2, 3)


def scores_of(keys, q):
    return lax.dot_general(keys, q, (((1,), (1,)), ((), ())), preferred_element_type=jnp.float32)


def top_of(load, pieces):
    top = load(0)
    for t in range(1, pieces):
        top = jnp.maximum(top, load(t))
    eight = top[0:8]
    for r in range(1, 8):
        eight = jnp.maximum(eight, top[8 * r : 8 * r + 8])
    return eight


def weigh(i, load, pieces, eight, values, top, tot, acc, start=False):
    new = jnp.broadcast_to(jnp.max(eight, axis=0, keepdims=True), eight.shape)
    if not start:
        old = top[i]
        new = jnp.maximum(old, new)
    level = new[0:1]
    rounded, part = [], None
    for t in range(pieces):
        weights = jnp.exp2((load(t) - level) * EXP2_SCALE)
        for r in range(8):
            piece = weights[8 * r : 8 * r + 8]
            part = piece if part is None else part + piece
        rounded.append(weights.astype(jnp.bfloat16))
    product = jnp.dot(values, jnp.concatenate(rounded, axis=0), preferred_element_type=jnp.float32)
    top[i] = new
    if start:
        tot[i] = part
        acc[i] = product
        return
    shrink = jnp.exp2((old - new) * EXP2_SCALE)
    tot[i] = tot[i] * shrink + part
    acc[i] = acc[i] * shrink[0:1] + product


def block_of(place_ref, i):
    return place_ref[0] * 16 + ((place_ref[1] - i // 4 + 4) % 4) * 4 + i % 4


def find_bounds(place_ref, bounds):
    bounds[0] = 0
    for g in range(1, 16):
        bounds[g] = row_rank(place_ref, 16 * g)
    bounds[16] = NV


def walk(place_ref, bounds, order, outer, at, sources, kc, vc):
    group, y, mine1, mine2, core = (place_ref[i] for i in range(5))
    second = (mine2 - outer + 4) % 4
    for inner in range(4):
        first = (mine1 - inner + 4) % 4
        g = jnp.where(core == 0, first * 4 + second, second * 4 + first)
        start = bounds[g]
        end = jnp.where(g <= group, bounds[g + 1], start)
        shift = at - start

        def one(entry, carry):
            block = place_ref[VERT + entry]
            to = entry + shift
            order[to] = block
            if sources is not None:
                source = sources[inner * len(sources) // 4]
                skip = inner % (4 // len(sources))
                slab = block // 4
                before = place_ref[VERT + jnp.maximum(entry - 1, 0)] // 4
                rank = jnp.where((entry > 0) & (before == slab), BLK, 0)
                row = (skip * 4 + (y - slab % 4 + 4) % 4) * 256 + rank
                rows = pl.ds(pl.multiple_of(to * BLK, BLK), BLK)
                kc[rows, :] = source[pl.ds(pl.multiple_of(row, BLK), BLK), :]
                vc[rows, :] = source[pl.ds(pl.multiple_of(row + 128, BLK), BLK), :]
            return carry

        lax.fori_loop(start, end, one, 0)
        at = at + end - start
    return at


def chunks(size, unroll, picks, place_ref, order, begin, count, ql, kc, vc, top, tot, acc, vt_ref, sa_ref, sb_ref, ma, mb):
    pieces = size // BLK
    vt, sa, sb = vt_ref.at[:, 0:size], sa_ref.at[0:size, :], sb_ref.at[0:size, :]

    total = 4 * len(picks)

    def query(m):
        if len(picks) == 4:
            return m
        return jnp.where(m < 4, 4 * picks[0], 4 * picks[1]) + m % 4

    def one_chunk(n, carry):
        first = begin + n * pieces
        rows = pl.ds(pl.multiple_of(first * BLK, HALF), size)
        last = order[first]
        for j in range(1, pieces):
            last = jnp.maximum(last, order[first + j])
        vt[...] = vc[rows, :].T

        def score(i, buffer, eight):
            scores = scores_of(kc[rows, :], ql[i])
            buffer[...] = scores
            eight[...] = top_of(lambda t: scores[BLK * t : BLK * (t + 1)], pieces)

        def run(masked):
            def finish(i, buffer, eight):
                def plain(t):
                    return buffer[BLK * t : BLK * (t + 1), :]

                if masked:
                    mine = block_of(place_ref, i)

                    def load(t):
                        return jnp.where(order[first + t] < mine, plain(t), NEGATIVE)

                    weigh(i, load, pieces, top_of(load, pieces), vt[...], top, tot, acc)
                else:
                    weigh(i, plain, pieces, eight[...], vt[...], top, tot, acc)

            score(query(0), sa, ma)
            score(query(1), sb, mb)
            each = 1 if masked else unroll

            def some(j, carry):
                for u in range(each):
                    m = 2 * (j * each + u)
                    finish(query(m), sa, ma)
                    score(query((m + 2) % total), sa, ma)
                    finish(query(m + 1), sb, mb)
                    score(query((m + 3) % total), sb, mb)
                return carry

            lax.fori_loop(0, total // (2 * each), some, 0)

        free = last < place_ref[0] * 16
        pl.when(free)(lambda: run(False))
        pl.when(jnp.logical_not(free))(lambda: run(True))
        return carry

    lax.fori_loop(0, count, one_chunk, 0)


def part_kernel(stage, picks, place_ref, *refs):
    splits = ((1,), (1, 1), (2,), ())[stage]
    sources, refs = refs[: sum(splits)], refs[sum(splits) :]
    ql = refs[0]
    refs = refs[6:] if stage else refs[4:]
    kc, vc, top, tot, acc = refs[:5]
    final = stage >= 2
    outs, refs = (refs[5 : 5 + len(picks)], refs[5 + len(picks) :]) if final else (None, refs[5:])
    bounds, order = refs[:2]
    work = (ql, kc, vc, top, tot, acc, *refs[2:])
    find_bounds(place_ref, bounds)

    def add(outer, at, fresh):
        return walk(place_ref, bounds, order, outer, at, fresh, kc, vc)

    near = add(0, jnp.int32(0), sources if stage == 0 else None)
    begin = near // 8 * 8
    if stage == 0:
        chunks(HALF, 2, picks, place_ref, order, jnp.int32(0), near // 8, *work)
        return
    at = add(1, near, sources[:1] if stage == 1 else None)
    at = add(3, at, sources[1:] if stage == 1 else None)
    whole = (at - begin) // 16
    if stage == 1:
        chunks(CHUNK, 2, picks, place_ref, order, begin, whole, *work)
        return
    at = add(2, at, sources if stage == 2 else None)
    begin = begin + whole * 16
    whole = (at - begin) // 16
    rest = begin + whole * 16
    left = (at - rest + 7) // 8

    def clear(n, carry):
        order[n] = NEVER
        vc[pl.ds(pl.multiple_of(n * BLK, BLK), BLK), :] = jnp.zeros((BLK, 128), jnp.bfloat16)
        return carry

    lax.fori_loop(at, rest + left * 8, clear, 0)
    chunks(CHUNK, 2, picks, place_ref, order, begin, whole, *work)
    chunks(HALF, 1, picks, place_ref, order, rest, left, *work)
    for out, by in zip(outs, picks):
        for block in range(4):
            i = by * 4 + block
            o = (acc[i] / jnp.sum(tot[i], axis=0, keepdims=True)).T.astype(jnp.bfloat16)
            for g in range(4):
                out[block * BLK : (block + 1) * BLK, g * 128 : (g + 1) * 128] = o[g * BLK : (g + 1) * BLK, :]


def local_kernel(
    place_ref, q0, q1, q2, q3, kv0, kv1, kv2, kv3, prev_ref, ql, top, tot, acc, kl, vl
):
    group, y = place_ref[0], place_ref[1]
    kl[0:SLAB, :] = prev_ref[:, 0:128]
    vl[0:SLAB, :] = prev_ref[:, 128:256]
    for by, (q, kv) in enumerate(((q0, kv0), (q1, kv1), (q2, kv2), (q3, kv3))):
        slab = (y - by + 4) % 4
        rows = pl.ds(pl.multiple_of(SLAB + slab * SLAB, SLAB), SLAB)
        kl[rows, :] = kv[:, 0:128]
        vl[rows, :] = kv[:, 128:256]
        for block in range(4):
            for g in range(4):
                ql[by * 4 + block, g * BLK : (g + 1) * BLK, :] = q[block * BLK : (block + 1) * BLK, g * 128 : (g + 1) * 128]
    key = lax.broadcasted_iota(jnp.int32, (BLK, 256), 0)
    row = lax.broadcasted_iota(jnp.int32, (BLK, 256), 1) % BLK

    def some(j, carry):
        ready = []
        for u in range(4):
            i = 4 * j + u
            block = block_of(place_ref, i)
            here = block - group * 16
            starts, valid = [here], []
            for s in range(2):
                offset = place_ref[SLASH + s]
                behind = block - offset
                at = jnp.minimum(row_rank(place_ref, behind), NV - 1)
                valid.append((behind >= 0) & (place_ref[VERT + at] != behind))
                starts.append(here - offset)
            rows = [pl.ds(pl.multiple_of(SLAB + at * BLK, BLK), BLK) for at in starts]
            keys = jnp.concatenate([kl[r, :] for r in rows] + [kl[rows[0], :]], axis=0)
            values = jnp.concatenate([vl[r, :] for r in rows] + [vl[rows[0], :]], axis=0).T
            ready.append((i, scores_of(keys, ql[i]), values, valid))
        for i, scores, values, valid in ready:
            def load(t):
                if t == 3:
                    return jnp.full((BLK, 256), NEGATIVE, jnp.float32)
                here = scores[BLK * t : BLK * (t + 1)]
                return jnp.where(key <= row if t == 0 else valid[t - 1], here, NEGATIVE)

            weigh(i, load, 4, top_of(load, 4), values, top, tot, acc, True)
        return carry

    lax.fori_loop(0, 4, some, 0)


def early_kernel(place_ref, a0, a1, a2, weight_ref, total_ref):
    for n in range(8):
        columns = slice(n * 512, (n + 1) * 512)
        total = None
        for by, a in enumerate((a0, a1, a2)):
            depth = pl.ds(pl.multiple_of((place_ref[1] + by) % 4 * 512, 512), 512)
            part = jnp.dot(a[...], weight_ref[depth, columns], preferred_element_type=jnp.float32)
            total = part if total is None else total + part
        total_ref[:, columns] = total


def last_kernel(mine, place_ref, a, weight_ref, total_ref, out_ref):
    core = place_ref[4]
    half = core if mine else 1 - core
    rows = pl.ds(pl.multiple_of(half * 128, 128), 128)
    depth = pl.ds(pl.multiple_of((place_ref[1] + 3) % 4 * 512, 512), 512)
    for n in range(8):
        columns = slice(n * 512, (n + 1) * 512)
        part = jnp.dot(a[rows, :], weight_ref[depth, columns], preferred_element_type=jnp.float32)
        out_ref[:, columns] = (total_ref[rows, columns] + part).astype(out_ref.dtype)


SMEM = pl.BlockSpec(memory_space=pltpu.SMEM)
VMEM = pl.BlockSpec(memory_space=pltpu.VMEM)


def bf16(*shape):
    return jax.ShapeDtypeStruct(shape, jnp.bfloat16)


def f32(*shape):
    return jax.ShapeDtypeStruct(shape, jnp.float32)


STATE = [f32(16, 8, 256), f32(16, 8, 256), f32(16, 128, 256)]
PACKED = [bf16(NV * BLK, 128)] * 2
WORK = [
    pltpu.SMEM((17,), jnp.int32),
    pltpu.SMEM((NV,), jnp.int32),
    pltpu.VMEM((128, CHUNK), jnp.bfloat16),
    pltpu.VMEM((CHUNK, 256), jnp.float32),
    pltpu.VMEM((CHUNK, 256), jnp.float32),
    pltpu.VMEM((8, 256), jnp.float32),
    pltpu.VMEM((8, 256), jnp.float32),
]


def call(kernel, outs, scalars, arrays, flops, limit, scratch=(), aliases=None, places=None):
    return pl.pallas_call(
        kernel,
        out_shape=outs,
        in_specs=[SMEM] * len(scalars) + [VMEM] * len(arrays),
        out_specs=places or [VMEM] * len(outs),
        scratch_shapes=list(scratch),
        input_output_aliases=aliases or {},
        compiler_params=pltpu.CompilerParams(vmem_limit_bytes=limit * MIB),
        cost_estimate=pl.CostEstimate(flops=int(flops), bytes_accessed=10**6, transcendentals=0),
    )(*scalars, *arrays)


def layer(queries, keys, values, vertical, slash, out_weight):
    x, z, y, c = (lax.axis_index(a) for a in ALL)
    place = jnp.stack([x * 4 + z, y, jnp.where(c == 0, x, z), jnp.where(c == 0, z, x), c]).astype(jnp.int32)
    kv = call(kv_kernel, [bf16(SLAB, 256)] * 4, [place], [keys, values], 1e6, 4)
    kv = [kv[0]] + [along_y(kv[by], by) for by in (1, 2, 3)]
    q = call(q_kernel, [bf16(SLAB, 512)] * 4, [place], [queries], 1e6, 4)
    q = [q[0]] + [along_y(q[by], by) for by in (1, 2, 3)]
    own, last, table = call(
        slots_kernel, [bf16(1024, 128), bf16(SLAB, 256), jax.ShapeDtypeStruct((128,), jnp.int32)],
        [place, vertical, slash.T], kv, 1e6, 4, (), None, [VMEM, VMEM, SMEM],
    )
    hops = [first_hop(own, by) for by in (1, 2, 3)]
    prev = to_next_group(last)
    near = call(join_kernel, [bf16(4096, 128)], [], [own, *hops], 1e6, 4)[0]
    plus, minus = second_hop(near, 1), second_hop(near, 3)
    beyond = [second_hop(plus[:2048], 1), second_hop(minus[2048:], 3)]
    ql, *state = call(
        local_kernel, [bf16(16, 256, 128)] + STATE, [table], [*q, *kv, prev], 3e9, 6,
        [pltpu.VMEM((5 * SLAB, 128), jnp.bfloat16)] * 2,
    )
    state = call(
        functools.partial(part_kernel, 0, EVERY), PACKED + STATE, [table],
        [near, ql, *state], 5e9, 8, WORK, {3 + n: 2 + n for n in range(3)},
    )
    state = call(
        functools.partial(part_kernel, 1, EVERY), PACKED + STATE, [table],
        [plus, minus, ql, *state], 1e10, 8, WORK, {4 + n: n for n in range(5)},
    )
    *state, a2, a1 = call(
        functools.partial(part_kernel, 2, (2, 1)), PACKED + STATE + [bf16(SLAB, 512)] * 2, [table],
        [*beyond, ql, *state], 3e9, 8, WORK, {4 + n: n for n in range(5)},
    )
    a2, a1 = along_y(a2, -2), along_y(a1, -1)
    *state, a3, a0 = call(
        functools.partial(part_kernel, 3, (3, 0)), PACKED + STATE + [bf16(SLAB, 512)] * 2, [table],
        [ql, *state], 3e9, 8, WORK, {2 + n: n for n in range(5)},
    )
    a3 = along_y(a3, -3)
    total = call(early_kernel, [f32(SLAB, 4096)], [place], [a0, a1, a2, out_weight], 3e9, 6)[0]
    theirs, mine = (
        call(functools.partial(last_kernel, own), [out], [place], [a3, out_weight, total], 1e9, 6)[0]
        for own, out in ((False, bf16(128, 4096)), (True, f32(128, 4096)))
    )
    other = to_partner(theirs)
    return (mine + other.astype(jnp.float32)).astype(jnp.bfloat16)


def solution(mesh):
    torus = Mesh(mesh.devices.reshape(4, 4, 4, 2), ALL)
    rows = ("x", "z", "y")
    placed = (P(rows, "c"), P(rows, "c"), P(rows, "c"), P("c", None), P("c", None), P("c", None))
    return jax.shard_map(layer, mesh=torus, in_specs=placed, out_specs=P(ALL, None), check_vma=False)
```

```python
import functools

import jax
import jax.numpy as jnp
from jax import lax
from jax.experimental import pallas as pl
from jax.experimental.pallas import tpu as pltpu
from jax.sharding import Mesh
from jax.sharding import PartitionSpec as P

HEAD_DIM = 128
BLK = 64
SLAB = 256
NV = 64
EXP2_SCALE = HEAD_DIM ** (-0.5) * 1.4426950408889634
NEGATIVE = -1e30
SLASH = 8
VERT = 16
NEVER = 1 << 20
BOUNDS = 96
ALL = ("x", "z", "y", "c")
MIB = 1 << 20


def moved(value, target):
    pairs = []
    for x in range(4):
        for z in range(4):
            for y in range(4):
                for c in range(2):
                    tx, tz, ty, tc = target(x, z, y, c)
                    pairs.append((((x * 4 + z) * 4 + y) * 2 + c, (((tx % 4) * 4 + tz % 4) * 4 + ty % 4) * 2 + tc))
    return lax.ppermute(value, ALL, pairs)


def along_y(value, by):
    return moved(value, lambda x, z, y, c: (x, z, y + by, c))


def first_hop(value, by):
    return moved(value, lambda x, z, y, c: (x + by, z, y, c) if c == 0 else (x, z + by, y, c))


def second_hop(value, by):
    return moved(value, lambda x, z, y, c: (x, z + by, y, c) if c == 0 else (x + by, z, y, c))


def to_next_group(value):
    return moved(value, lambda x, z, y, c: (x + (z + 1) // 4, z + 1, y, c))


def to_partner(value):
    return moved(value, lambda x, z, y, c: (x, z, y, 1 - c))


def row_rank(table_ref, block):
    at = jnp.int32(VERT)
    for width in (32, 16, 8, 4, 2, 1):
        at = at + jnp.where(table_ref[at + width - 1] < block, width, 0)
    return at - VERT + jnp.where(table_ref[at] < block, 1, 0)


def kv_kernel(place_ref, keys_ref, values_ref, *out_refs):
    y = place_ref[1]
    for by in range(4):
        lanes = pl.ds(pl.multiple_of((y + by) % 4 * HEAD_DIM, HEAD_DIM), HEAD_DIM)
        out_refs[by][:, 0:128] = keys_ref[:, lanes]
        out_refs[by][:, 128:256] = values_ref[:, lanes]


def q_kernel(place_ref, queries_ref, *out_refs):
    y = place_ref[1]
    for by in range(4):
        out_refs[by][...] = queries_ref[:, pl.ds(pl.multiple_of((y + by) % 4 * 512, 512), 512)]


def slots_kernel(place_ref, vert_ref, slash_ref, kv0, kv1, kv2, kv3, own_ref, last_ref, table_ref):
    group, y = place_ref[0], place_ref[1]
    for n in range(5):
        table_ref[n] = place_ref[n]
    for n in range(2):
        table_ref[SLASH + n] = slash_ref[n, y]
    for n in range(NV):
        table_ref[VERT + n] = vert_ref[y, n]
    for by, kv in enumerate((kv0, kv1, kv2, kv3)):
        slab = (y - by + 4) % 4
        first = (group * 4 + slab) * 4
        at = row_rank(table_ref, first)
        for slot in range(2):
            entry = jnp.minimum(at + slot, NV - 1)
            block = table_ref[VERT + entry] - first
            block = jnp.where((block >= 0) & (block < 4), block, 0)
            rows = pl.ds(pl.multiple_of(block * BLK, BLK), BLK)
            to = by * 256 + slot * BLK
            own_ref[to : to + BLK, :] = kv[rows, 0:128]
            own_ref[to + 128 : to + 128 + BLK, :] = kv[rows, 128:256]

        @pl.when(slab == 3)
        def _():
            last_ref[...] = kv[...]


def join_kernel(a0, a1, a2, a3, out_ref):
    for n, a in enumerate((a0, a1, a2, a3)):
        out_ref[n * 1024 : (n + 1) * 1024, :] = a[...]


CHUNK = 1024
HALF = 512
EVERY = (0, 1, 2, 3)


def scores_of(keys, q):
    return lax.dot_general(keys, q, (((1,), (1,)), ((), ())), preferred_element_type=jnp.float32)


def top_of(load, pieces):
    top = load(0)
    for t in range(1, pieces):
        top = jnp.maximum(top, load(t))
    eight = top[0:8]
    for r in range(1, 8):
        eight = jnp.maximum(eight, top[8 * r : 8 * r + 8])
    return eight


def weigh(i, load, pieces, eight, values, top, tot, acc, start=False):
    new = jnp.broadcast_to(jnp.max(eight, axis=0, keepdims=True), eight.shape)
    if not start:
        old = top[i]
        new = jnp.maximum(old, new)
    level = new[0:1]
    rounded, part = [], None
    for t in range(pieces):
        weights = jnp.exp2((load(t) - level) * EXP2_SCALE)
        for r in range(8):
            piece = weights[8 * r : 8 * r + 8]
            part = piece if part is None else part + piece
        rounded.append(weights.astype(jnp.bfloat16))
    product = jnp.dot(values, jnp.concatenate(rounded, axis=0), preferred_element_type=jnp.float32)
    top[i] = new
    if start:
        tot[i] = part
        acc[i] = product
        return
    shrink = jnp.exp2((old - new) * EXP2_SCALE)
    tot[i] = tot[i] * shrink + part
    acc[i] = acc[i] * shrink[0:1] + product


def block_of(place_ref, i):
    return place_ref[0] * 16 + ((place_ref[1] - i // 4 + 4) % 4) * 4 + i % 4


def count_of(table_ref, outer):
    total = jnp.int32(0)
    for inner in range(4):
        start, end = span_of(table_ref, outer, inner)
        total = total + end - start
    return total


def span_of(table_ref, outer, inner):
    group, core = table_ref[0], table_ref[4]
    first = (table_ref[2] - inner + 4) % 4
    second = (table_ref[3] - outer + 4) % 4
    g = jnp.where(core == 0, first * 4 + second, second * 4 + first)
    start = table_ref[BOUNDS + g]
    return start, jnp.where(g < group, table_ref[BOUNDS + g + 1], start)


def pack(table_ref, start, end, at, source, base, kc, vc):
    y = table_ref[1]

    def one(entry, carry):
        slab = table_ref[VERT + entry] // 4
        before = table_ref[VERT + jnp.maximum(entry - 1, 0)] // 4
        rank = jnp.where((entry > 0) & (before == slab), BLK, 0)
        row = (base * 4 + (y - slab % 4 + 4) % 4) * 256 + rank
        rows = pl.ds(pl.multiple_of((at + entry - start) * BLK, BLK), BLK)
        kc[rows, :] = source[pl.ds(pl.multiple_of(row, BLK), BLK), :]
        vc[rows, :] = source[pl.ds(pl.multiple_of(row + 128, BLK), BLK), :]
        return carry

    lax.fori_loop(start, end, one, 0)
    return at + end - start


def pack_all(table_ref, outer, at, sources, kc, vc):
    for inner in range(4):
        start, end = span_of(table_ref, outer, inner)
        part = 4 // len(sources)
        at = pack(table_ref, start, end, at, sources[inner // part], inner % part, kc, vc)
    return at


def chunks(size, each, masked, picks, table_ref, order, begin, count, ql, kc, vc, top, tot, acc, vt_ref, sa_ref, sb_ref, ma, mb):
    pieces = size // BLK
    vt, sa, sb = vt_ref.at[:, 0:size], sa_ref.at[0:size, :], sb_ref.at[0:size, :]
    total = 4 * len(picks)

    def query(m):
        if len(picks) == 4:
            return m
        return jnp.where(m < 4, 4 * picks[0], 4 * picks[1]) + m % 4

    def one_chunk(n, carry):
        first = begin + n * pieces
        rows = pl.ds(pl.multiple_of(first * BLK, HALF), size)
        vt[...] = vc[rows, :].T

        def score(i, buffer, eight):
            scores = scores_of(kc[rows, :], ql[i])
            if masked:
                mine = block_of(table_ref, i)
                scores = jnp.concatenate(
                    [
                        jnp.where(order[first + t] < mine, scores[BLK * t : BLK * (t + 1)], NEGATIVE)
                        for t in range(pieces)
                    ],
                    axis=0,
                )
            buffer[...] = scores
            eight[...] = top_of(lambda t: scores[BLK * t : BLK * (t + 1)], pieces)

        def finish(i, buffer, eight):
            weigh(i, lambda t: buffer[BLK * t : BLK * (t + 1), :], pieces, eight[...], vt[...], top, tot, acc)

        score(query(0), sa, ma)
        score(query(1), sb, mb)

        def some(j, carry):
            for u in range(each):
                m = 2 * (j * each + u)
                finish(query(m), sa, ma)
                score(query((m + 2) % total), sa, ma)
                finish(query(m + 1), sb, mb)
                score(query((m + 3) % total), sb, mb)
            return carry

        lax.fori_loop(0, total // (2 * each), some, 0)
        return carry

    lax.fori_loop(0, count, one_chunk, 0)


def part_kernel(stage, picks, table_ref, *refs):
    splits = ((1,), (1, 1), (2,), ())[stage]
    sources, refs = refs[: sum(splits)], refs[sum(splits) :]
    ql = refs[0]
    refs = refs[6:] if stage else refs[4:]
    kc, vc, top, tot, acc = refs[:5]
    final = stage >= 2
    outs, refs = (refs[5 : 5 + len(picks)], refs[5 + len(picks) :]) if final else (None, refs[5:])
    order = refs[0]
    work = (ql, kc, vc, top, tot, acc, *refs[1:])
    others, total = table_ref[BOUNDS + table_ref[0]], table_ref[BOUNDS + table_ref[0] + 1]
    near = count_of(table_ref, 0)
    begin = jnp.minimum(near // 8, 2) * 8
    if stage == 0:
        pack_all(table_ref, 0, jnp.int32(0), sources, kc, vc)
        pack(table_ref, others, total, others, sources[0], 0, kc, vc)
        chunks(HALF, 2, False, picks, table_ref, order, jnp.int32(0), begin // 8, *work)
        return
    if stage == 1:
        at = pack_all(table_ref, 1, near, sources[:1], kc, vc)
        at = pack_all(table_ref, 3, at, sources[1:], kc, vc)
        chunks(CHUNK, 4, False, picks, table_ref, order, begin, (at - begin) // 16, *work)
        return
    at = near + count_of(table_ref, 1) + count_of(table_ref, 3)
    begin = begin + (at - begin) // 16 * 16
    whole = (others - begin) // 16
    half = begin + whole * 16
    halves = (others - half) // 8
    rest = half + halves * 8
    left = (total - rest + 7) // 8
    if stage == 2:
        pack_all(table_ref, 2, at, sources, kc, vc)

    def mark(n, carry):
        own = table_ref[VERT + jnp.minimum(n, NV - 1)]
        order[n] = jnp.where(n < others, -1, jnp.where(n < total, own, NEVER))

        @pl.when(n >= total)
        def _():
            vc[pl.ds(pl.multiple_of(n * BLK, BLK), BLK), :] = jnp.zeros((BLK, 128), jnp.bfloat16)

        return carry

    lax.fori_loop(rest, rest + left * 8, mark, 0)
    chunks(CHUNK, 4, False, picks, table_ref, order, begin, whole, *work)
    chunks(HALF, 2, False, picks, table_ref, order, half, halves, *work)
    chunks(HALF, 1, True, picks, table_ref, order, rest, left, *work)
    for out, by in zip(outs, picks):
        for block in range(4):
            i = by * 4 + block
            o = (acc[i] / jnp.sum(tot[i], axis=0, keepdims=True)).T.astype(jnp.bfloat16)
            for g in range(4):
                out[block * BLK : (block + 1) * BLK, g * 128 : (g + 1) * 128] = o[g * BLK : (g + 1) * BLK, :]


def local_kernel(
    place_ref, q0, q1, q2, q3, kv0, kv1, kv2, kv3, prev_ref, ql, top, tot, acc, table_ref, kl, vl
):
    group, y = place_ref[0], place_ref[1]
    for n in range(VERT + NV):
        table_ref[n] = place_ref[n]
    table_ref[BOUNDS] = 0
    for g in range(1, 16):
        table_ref[BOUNDS + g] = row_rank(place_ref, 16 * g)
    table_ref[BOUNDS + 16] = NV
    kl[0:SLAB, :] = prev_ref[:, 0:128]
    vl[0:SLAB, :] = prev_ref[:, 128:256]
    for by, (q, kv) in enumerate(((q0, kv0), (q1, kv1), (q2, kv2), (q3, kv3))):
        slab = (y - by + 4) % 4
        rows = pl.ds(pl.multiple_of(SLAB + slab * SLAB, SLAB), SLAB)
        kl[rows, :] = kv[:, 0:128]
        vl[rows, :] = kv[:, 128:256]
        for block in range(4):
            for g in range(4):
                ql[by * 4 + block, g * BLK : (g + 1) * BLK, :] = q[block * BLK : (block + 1) * BLK, g * 128 : (g + 1) * 128]
    key = lax.broadcasted_iota(jnp.int32, (BLK, 256), 0)
    row = lax.broadcasted_iota(jnp.int32, (BLK, 256), 1) % BLK

    def some(j, carry):
        ready = []
        for u in range(4):
            i = 4 * j + u
            block = block_of(place_ref, i)
            here = block - group * 16
            starts, valid = [here], []
            for s in range(2):
                offset = place_ref[SLASH + s]
                behind = block - offset
                at = jnp.minimum(row_rank(place_ref, behind), NV - 1)
                valid.append((behind >= 0) & (place_ref[VERT + at] != behind))
                starts.append(here - offset)
            rows = [pl.ds(pl.multiple_of(SLAB + at * BLK, BLK), BLK) for at in starts]
            keys = jnp.concatenate([kl[r, :] for r in rows] + [kl[rows[0], :]], axis=0)
            values = jnp.concatenate([vl[r, :] for r in rows] + [vl[rows[0], :]], axis=0).T
            ready.append((i, scores_of(keys, ql[i]), values, valid))
        for i, scores, values, valid in ready:
            def load(t):
                if t == 3:
                    return jnp.full((BLK, 256), NEGATIVE, jnp.float32)
                here = scores[BLK * t : BLK * (t + 1)]
                return jnp.where(key <= row if t == 0 else valid[t - 1], here, NEGATIVE)

            weigh(i, load, 4, top_of(load, 4), values, top, tot, acc, True)
        return carry

    lax.fori_loop(0, 4, some, 0)


def early_kernel(place_ref, a0, a1, a2, weight_ref, total_ref):
    for n in range(8):
        columns = slice(n * 512, (n + 1) * 512)
        total = None
        for by, a in enumerate((a0, a1, a2)):
            depth = pl.ds(pl.multiple_of((place_ref[1] + by) % 4 * 512, 512), 512)
            part = jnp.dot(a[...], weight_ref[depth, columns], preferred_element_type=jnp.float32)
            total = part if total is None else total + part
        total_ref[:, columns] = total


def last_kernel(mine, place_ref, a, weight_ref, total_ref, out_ref):
    core = place_ref[4]
    half = core if mine else 1 - core
    rows = pl.ds(pl.multiple_of(half * 128, 128), 128)
    depth = pl.ds(pl.multiple_of((place_ref[1] + 3) % 4 * 512, 512), 512)
    for n in range(8):
        columns = slice(n * 512, (n + 1) * 512)
        part = jnp.dot(a[rows, :], weight_ref[depth, columns], preferred_element_type=jnp.float32)
        out_ref[:, columns] = (total_ref[rows, columns] + part).astype(out_ref.dtype)


SMEM = pl.BlockSpec(memory_space=pltpu.SMEM)
VMEM = pl.BlockSpec(memory_space=pltpu.VMEM)


def bf16(*shape):
    return jax.ShapeDtypeStruct(shape, jnp.bfloat16)


def f32(*shape):
    return jax.ShapeDtypeStruct(shape, jnp.float32)


TABLE = jax.ShapeDtypeStruct((128,), jnp.int32)
STATE = [f32(16, 8, 256), f32(16, 8, 256), f32(16, 128, 256)]
PACKED = [bf16(NV * BLK, 128)] * 2
WORK = [
    pltpu.SMEM((NV + 8,), jnp.int32),
    pltpu.VMEM((128, CHUNK), jnp.bfloat16),
    pltpu.VMEM((CHUNK, 256), jnp.float32),
    pltpu.VMEM((CHUNK, 256), jnp.float32),
    pltpu.VMEM((8, 256), jnp.float32),
    pltpu.VMEM((8, 256), jnp.float32),
]


def call(kernel, outs, scalars, arrays, flops, limit, scratch=(), aliases=None, places=None):
    return pl.pallas_call(
        kernel,
        out_shape=outs,
        in_specs=[SMEM] * len(scalars) + [VMEM] * len(arrays),
        out_specs=places or [VMEM] * len(outs),
        scratch_shapes=list(scratch),
        input_output_aliases=aliases or {},
        compiler_params=pltpu.CompilerParams(vmem_limit_bytes=limit * MIB),
        cost_estimate=pl.CostEstimate(flops=int(flops), bytes_accessed=10**6, transcendentals=0),
    )(*scalars, *arrays)


def layer(queries, keys, values, vertical, slash, out_weight):
    x, z, y, c = (lax.axis_index(a) for a in ALL)
    place = jnp.stack([x * 4 + z, y, jnp.where(c == 0, x, z), jnp.where(c == 0, z, x), c]).astype(jnp.int32)
    kv = call(kv_kernel, [bf16(SLAB, 256)] * 4, [place], [keys, values], 1e6, 4)
    kv = [kv[0]] + [along_y(kv[by], by) for by in (1, 2, 3)]
    q = call(q_kernel, [bf16(SLAB, 512)] * 4, [place], [queries], 1e6, 4)
    q = [q[0]] + [along_y(q[by], by) for by in (1, 2, 3)]
    own, last, table = call(
        slots_kernel, [bf16(1024, 128), bf16(SLAB, 256), TABLE],
        [place, vertical, slash.T], kv, 1e6, 4, (), None, [VMEM, VMEM, SMEM],
    )
    hops = [first_hop(own, by) for by in (1, 2, 3)]
    prev = to_next_group(last)
    near = call(join_kernel, [bf16(4096, 128)], [], [own, *hops], 1e6, 4)[0]
    plus, minus = second_hop(near, 1), second_hop(near, 3)
    beyond = [second_hop(plus[:2048], 1), second_hop(minus[2048:], 3)]
    ql, *state, table = call(
        local_kernel, [bf16(16, 256, 128)] + STATE + [TABLE], [table], [*q, *kv, prev], 3e9, 6,
        [pltpu.VMEM((5 * SLAB, 128), jnp.bfloat16)] * 2, None, [VMEM] * 4 + [SMEM],
    )
    state = call(
        functools.partial(part_kernel, 0, EVERY), PACKED + STATE, [table],
        [near, ql, *state], 5e9, 8, WORK, {3 + n: 2 + n for n in range(3)},
    )
    state = call(
        functools.partial(part_kernel, 1, EVERY), PACKED + STATE, [table],
        [plus, minus, ql, *state], 1e10, 8, WORK, {4 + n: n for n in range(5)},
    )
    *state, a2, a1 = call(
        functools.partial(part_kernel, 2, (2, 1)), PACKED + STATE + [bf16(SLAB, 512)] * 2, [table],
        [*beyond, ql, *state], 3e9, 8, WORK, {4 + n: n for n in range(5)},
    )
    a2, a1 = along_y(a2, -2), along_y(a1, -1)
    *state, a3, a0 = call(
        functools.partial(part_kernel, 3, (3, 0)), PACKED + STATE + [bf16(SLAB, 512)] * 2, [table],
        [ql, *state], 3e9, 8, WORK, {2 + n: n for n in range(5)},
    )
    a3 = along_y(a3, -3)
    total = call(early_kernel, [f32(SLAB, 4096)], [place], [a0, a1, a2, out_weight], 3e9, 6)[0]
    theirs, mine = (
        call(functools.partial(last_kernel, own), [out], [place], [a3, out_weight, total], 1e9, 6)[0]
        for own, out in ((False, bf16(128, 4096)), (True, f32(128, 4096)))
    )
    other = to_partner(theirs)
    return (mine + other.astype(jnp.float32)).astype(jnp.bfloat16)


def solution(mesh):
    torus = Mesh(mesh.devices.reshape(4, 4, 4, 2), ALL)
    rows = ("x", "z", "y")
    placed = (P(rows, "c"), P(rows, "c"), P(rows, "c"), P("c", None), P("c", None), P("c", None))
    return jax.shard_map(layer, mesh=torus, in_specs=placed, out_specs=P(ALL, None), check_vma=False)
```

```python
import functools

import jax
import jax.numpy as jnp
from jax import lax
from jax.experimental import pallas as pl
from jax.experimental.pallas import tpu as pltpu
from jax.sharding import Mesh
from jax.sharding import PartitionSpec as P

HEAD_DIM = 128
BLK = 64
SLAB = 256
NV = 64
EXP2_SCALE = HEAD_DIM ** (-0.5) * 1.4426950408889634
NEGATIVE = -1e30
SLASH = 8
VERT = 16
NEVER = 1 << 20
BOUNDS = 96
ALL = ("x", "z", "y", "c")
MIB = 1 << 20


def moved(value, target):
    pairs = []
    for x in range(4):
        for z in range(4):
            for y in range(4):
                for c in range(2):
                    tx, tz, ty, tc = target(x, z, y, c)
                    pairs.append((((x * 4 + z) * 4 + y) * 2 + c, (((tx % 4) * 4 + tz % 4) * 4 + ty % 4) * 2 + tc))
    return lax.ppermute(value, ALL, pairs)


def along_y(value, by):
    return moved(value, lambda x, z, y, c: (x, z, y + by, c))


def first_hop(value, by):
    return moved(value, lambda x, z, y, c: (x + by, z, y, c) if c == 0 else (x, z + by, y, c))


def second_hop(value, by):
    return moved(value, lambda x, z, y, c: (x, z + by, y, c) if c == 0 else (x + by, z, y, c))


def to_next_group(value):
    return moved(value, lambda x, z, y, c: (x + (z + 1) // 4, z + 1, y, c))


def to_partner(value):
    return moved(value, lambda x, z, y, c: (x, z, y, 1 - c))


def row_rank(table_ref, block):
    at = jnp.int32(VERT)
    for width in (32, 16, 8, 4, 2, 1):
        at = at + jnp.where(table_ref[at + width - 1] < block, width, 0)
    return at - VERT + jnp.where(table_ref[at] < block, 1, 0)


def kv_kernel(place_ref, keys_ref, values_ref, *out_refs):
    y = place_ref[1]
    for by in range(4):
        lanes = pl.ds(pl.multiple_of((y + by) % 4 * HEAD_DIM, HEAD_DIM), HEAD_DIM)
        out_refs[by][:, 0:128] = keys_ref[:, lanes]
        out_refs[by][:, 128:256] = values_ref[:, lanes]


def q_kernel(place_ref, queries_ref, *out_refs):
    y = place_ref[1]
    for by in range(4):
        out_refs[by][...] = queries_ref[:, pl.ds(pl.multiple_of((y + by) % 4 * 512, 512), 512)]


def table_kernel(place_ref, vert_ref, slash_ref, table_ref):
    y = place_ref[1]
    for n in range(5):
        table_ref[n] = place_ref[n]
    for n in range(2):
        table_ref[SLASH + n] = slash_ref[n, y]
    for n in range(NV):
        table_ref[VERT + n] = vert_ref[y, n]


def slots_kernel(table_ref, kv0, kv1, kv2, kv3, own_ref, last_ref):
    group, y = table_ref[0], table_ref[1]
    for by, kv in enumerate((kv0, kv1, kv2, kv3)):
        slab = (y - by + 4) % 4
        first = (group * 4 + slab) * 4
        at = row_rank(table_ref, first)
        for slot in range(2):
            entry = jnp.minimum(at + slot, NV - 1)
            block = table_ref[VERT + entry] - first
            block = jnp.where((block >= 0) & (block < 4), block, 0)
            rows = pl.ds(pl.multiple_of(block * BLK, BLK), BLK)
            to = by * 256 + slot * BLK
            own_ref[to : to + BLK, :] = kv[rows, 0:128]
            own_ref[to + 128 : to + 128 + BLK, :] = kv[rows, 128:256]

        @pl.when(slab == 3)
        def _():
            last_ref[...] = kv[...]


def join_kernel(a0, a1, a2, a3, out_ref):
    for n, a in enumerate((a0, a1, a2, a3)):
        out_ref[n * 1024 : (n + 1) * 1024, :] = a[...]


CHUNK = 1024
HALF = 512
EVERY = (0, 1, 2, 3)


def scores_of(keys, q):
    return lax.dot_general(keys, q, (((1,), (1,)), ((), ())), preferred_element_type=jnp.float32)


def top_of(load, pieces):
    top = load(0)
    for t in range(1, pieces):
        top = jnp.maximum(top, load(t))
    eight = top[0:8]
    for r in range(1, 8):
        eight = jnp.maximum(eight, top[8 * r : 8 * r + 8])
    return eight


def weigh(i, load, pieces, eight, values, top, tot, acc, start=False):
    new = jnp.broadcast_to(jnp.max(eight, axis=0, keepdims=True), eight.shape)
    if not start:
        old = top[i]
        new = jnp.maximum(old, new)
    level = new[0:1]
    rounded, part = [], None
    for t in range(pieces):
        weights = jnp.exp2((load(t) - level) * EXP2_SCALE)
        for r in range(8):
            piece = weights[8 * r : 8 * r + 8]
            part = piece if part is None else part + piece
        rounded.append(weights.astype(jnp.bfloat16))
    product = jnp.dot(values, jnp.concatenate(rounded, axis=0), preferred_element_type=jnp.float32)
    top[i] = new
    if start:
        tot[i] = part
        acc[i] = product
        return
    shrink = jnp.exp2((old - new) * EXP2_SCALE)
    tot[i] = tot[i] * shrink + part
    acc[i] = acc[i] * shrink[0:1] + product


def block_of(place_ref, i):
    return place_ref[0] * 16 + ((place_ref[1] - i // 4 + 4) % 4) * 4 + i % 4


def count_of(table_ref, outer):
    total = jnp.int32(0)
    for inner in range(4):
        start, end = span_of(table_ref, outer, inner)
        total = total + end - start
    return total


def span_of(table_ref, outer, inner):
    group, core = table_ref[0], table_ref[4]
    first = (table_ref[2] - inner + 4) % 4
    second = (table_ref[3] - outer + 4) % 4
    g = jnp.where(core == 0, first * 4 + second, second * 4 + first)
    start = table_ref[BOUNDS + g]
    return start, jnp.where(g < group, table_ref[BOUNDS + g + 1], start)


def pack(table_ref, start, end, at, source, base, kc, vc):
    y = table_ref[1]

    def one(entry, carry):
        slab = table_ref[VERT + entry] // 4
        before = table_ref[VERT + jnp.maximum(entry - 1, 0)] // 4
        rank = jnp.where((entry > 0) & (before == slab), BLK, 0)
        row = (base * 4 + (y - slab % 4 + 4) % 4) * 256 + rank
        rows = pl.ds(pl.multiple_of((at + entry - start) * BLK, BLK), BLK)
        kc[rows, :] = source[pl.ds(pl.multiple_of(row, BLK), BLK), :]
        vc[rows, :] = source[pl.ds(pl.multiple_of(row + 128, BLK), BLK), :]
        return carry

    lax.fori_loop(start, end, one, 0)
    return at + end - start


def pack_all(table_ref, outer, at, sources, kc, vc):
    for inner in range(4):
        start, end = span_of(table_ref, outer, inner)
        part = 4 // len(sources)
        at = pack(table_ref, start, end, at, sources[inner // part], inner % part, kc, vc)
    return at


def chunks(size, each, masked, picks, table_ref, order, begin, count, ql, kc, vc, top, tot, acc, vt_ref, sa_ref, sb_ref, ma, mb):
    pieces = size // BLK
    vt, sa, sb = vt_ref.at[:, 0:size], sa_ref.at[0:size, :], sb_ref.at[0:size, :]
    total = 4 * len(picks)
    steps = total // (2 * each)

    def query(m):
        if len(picks) == 4:
            return m
        if len(picks) == 1:
            return 4 * picks[0] + m
        return jnp.where(m < 4, 4 * picks[0], 4 * picks[1]) + m % 4

    def one_chunk(n, carry):
        first = begin + n * pieces
        rows = pl.ds(pl.multiple_of(first * BLK, HALF), size)
        vt[...] = vc[rows, :].T

        def score(i, buffer, eight):
            scores = scores_of(kc[rows, :], ql[i])
            if masked:
                mine = block_of(table_ref, i)
                scores = jnp.concatenate(
                    [
                        jnp.where(order[first + t] < mine, scores[BLK * t : BLK * (t + 1)], NEGATIVE)
                        for t in range(pieces)
                    ],
                    axis=0,
                )
            buffer[...] = scores
            eight[...] = top_of(lambda t: scores[BLK * t : BLK * (t + 1)], pieces)

        def finish(i, buffer, eight):
            weigh(i, lambda t: buffer[BLK * t : BLK * (t + 1), :], pieces, eight[...], vt[...], top, tot, acc)

        score(query(0), sa, ma)
        score(query(1), sb, mb)

        def some(j, carry):
            for u in range(each):
                m = 2 * (j * each + u)
                more = steps > 1 or u < each - 1
                finish(query(m), sa, ma)
                if more:
                    score(query((m + 2) % total), sa, ma)
                finish(query(m + 1), sb, mb)
                if more:
                    score(query((m + 3) % total), sb, mb)
            return carry

        if steps == 1:
            some(0, 0)
        else:
            lax.fori_loop(0, steps, some, 0)
        return carry

    lax.fori_loop(0, count, one_chunk, 0)


def part_kernel(stage, picks, table_ref, *refs):
    splits = ((1, 1), (2,), ())[stage]
    sources, refs = refs[: sum(splits)], refs[sum(splits) :]
    ql, refs = refs[0], refs[6:]
    kc, vc, top, tot, acc = refs[:5]
    outs, refs = (refs[5 : 5 + len(picks)], refs[5 + len(picks) :]) if stage else (None, refs[5:])
    order = refs[0]
    work = (ql, kc, vc, top, tot, acc, *refs[1:])
    others, total = table_ref[BOUNDS + table_ref[0]], table_ref[BOUNDS + table_ref[0] + 1]
    at = count_of(table_ref, 0)
    if stage == 0:
        at = pack_all(table_ref, 1, at, sources[:1], kc, vc)
        at = pack_all(table_ref, 3, at, sources[1:], kc, vc)
        chunks(CHUNK, 4, False, picks, table_ref, order, jnp.int32(0), at // 16, *work)
        return
    at = at + count_of(table_ref, 1) + count_of(table_ref, 3)
    begin = at // 16 * 16
    whole = (others - begin) // 16
    rest = begin + whole * 16
    left = (total - rest + 7) // 8
    if stage == 1:
        pack_all(table_ref, 2, at, sources, kc, vc)

    def mark(n, carry):
        own = table_ref[VERT + jnp.minimum(n, NV - 1)]
        order[n] = jnp.where(n < others, -1, jnp.where(n < total, own, NEVER))

        @pl.when(n >= total)
        def _():
            vc[pl.ds(pl.multiple_of(n * BLK, BLK), BLK), :] = jnp.zeros((BLK, 128), jnp.bfloat16)

        return carry

    lax.fori_loop(rest, rest + left * 8, mark, 0)
    chunks(CHUNK, 2 * len(picks), False, picks, table_ref, order, begin, whole, *work)
    chunks(HALF, 2 * len(picks), True, picks, table_ref, order, rest, left, *work)
    for out, by in zip(outs, picks):
        for block in range(4):
            i = by * 4 + block
            o = (acc[i] / jnp.sum(tot[i], axis=0, keepdims=True)).T.astype(jnp.bfloat16)
            for g in range(4):
                out[block * BLK : (block + 1) * BLK, g * 128 : (g + 1) * 128] = o[g * BLK : (g + 1) * BLK, :]


def local_kernel(
    place_ref, q0, q1, q2, q3, kv0, kv1, kv2, kv3, prev_ref, near,
    ql, kc, vc, top, tot, acc, table_ref, kl, vl
):
    group, y = place_ref[0], place_ref[1]
    for n in range(VERT + NV):
        table_ref[n] = place_ref[n]
    table_ref[BOUNDS] = 0
    for g in range(1, 16):
        table_ref[BOUNDS + g] = row_rank(place_ref, 16 * g)
    table_ref[BOUNDS + 16] = NV
    kl[0:SLAB, :] = prev_ref[:, 0:128]
    vl[0:SLAB, :] = prev_ref[:, 128:256]
    for by, (q, kv) in enumerate(((q0, kv0), (q1, kv1), (q2, kv2), (q3, kv3))):
        slab = (y - by + 4) % 4
        rows = pl.ds(pl.multiple_of(SLAB + slab * SLAB, SLAB), SLAB)
        kl[rows, :] = kv[:, 0:128]
        vl[rows, :] = kv[:, 128:256]
        for block in range(4):
            for g in range(4):
                ql[by * 4 + block, g * BLK : (g + 1) * BLK, :] = q[block * BLK : (block + 1) * BLK, g * 128 : (g + 1) * 128]
    key = lax.broadcasted_iota(jnp.int32, (BLK, 256), 0)
    row = lax.broadcasted_iota(jnp.int32, (BLK, 256), 1) % BLK

    def some(j, carry):
        ready = []
        for u in range(4):
            i = 4 * j + u
            block = block_of(place_ref, i)
            here = block - group * 16
            starts, valid = [here], []
            for s in range(2):
                offset = place_ref[SLASH + s]
                behind = block - offset
                at = jnp.minimum(row_rank(place_ref, behind), NV - 1)
                valid.append((behind >= 0) & (place_ref[VERT + at] != behind))
                starts.append(here - offset)
            rows = [pl.ds(pl.multiple_of(SLAB + at * BLK, BLK), BLK) for at in starts]
            keys = jnp.concatenate([kl[r, :] for r in rows] + [kl[rows[0], :]], axis=0)
            values = jnp.concatenate([vl[r, :] for r in rows] + [vl[rows[0], :]], axis=0).T
            ready.append((i, scores_of(keys, ql[i]), values, valid))
        for i, scores, values, valid in ready:
            def load(t):
                if t == 3:
                    return jnp.full((BLK, 256), NEGATIVE, jnp.float32)
                here = scores[BLK * t : BLK * (t + 1)]
                return jnp.where(key <= row if t == 0 else valid[t - 1], here, NEGATIVE)

            weigh(i, load, 4, top_of(load, 4), values, top, tot, acc, True)
        return carry

    lax.fori_loop(0, 4, some, 0)
    pack_all(table_ref, 0, jnp.int32(0), [near], kc, vc)
    others, total = table_ref[BOUNDS + group], table_ref[BOUNDS + group + 1]
    pack(table_ref, others, total, others, near, 0, kc, vc)


def early_kernel(place_ref, a0, a1, a2, weight_ref, total_ref):
    for n in range(8):
        columns = slice(n * 512, (n + 1) * 512)
        total = None
        for by, a in enumerate((a0, a1, a2)):
            depth = pl.ds(pl.multiple_of((place_ref[1] + by) % 4 * 512, 512), 512)
            part = jnp.dot(a[...], weight_ref[depth, columns], preferred_element_type=jnp.float32)
            total = part if total is None else total + part
        total_ref[:, columns] = total


def last_kernel(mine, place_ref, a, weight_ref, total_ref, out_ref):
    core = place_ref[4]
    half = core if mine else 1 - core
    rows = pl.ds(pl.multiple_of(half * 128, 128), 128)
    depth = pl.ds(pl.multiple_of((place_ref[1] + 3) % 4 * 512, 512), 512)
    for n in range(8):
        columns = slice(n * 512, (n + 1) * 512)
        part = jnp.dot(a[rows, :], weight_ref[depth, columns], preferred_element_type=jnp.float32)
        out_ref[:, columns] = (total_ref[rows, columns] + part).astype(out_ref.dtype)


SMEM = pl.BlockSpec(memory_space=pltpu.SMEM)
VMEM = pl.BlockSpec(memory_space=pltpu.VMEM)


def bf16(*shape):
    return jax.ShapeDtypeStruct(shape, jnp.bfloat16)


def f32(*shape):
    return jax.ShapeDtypeStruct(shape, jnp.float32)


TABLE = jax.ShapeDtypeStruct((128,), jnp.int32)
STATE = [f32(16, 8, 256), f32(16, 8, 256), f32(16, 128, 256)]
PACKED = [bf16(NV * BLK, 128)] * 2
WORK = [
    pltpu.SMEM((NV + 8,), jnp.int32),
    pltpu.VMEM((128, CHUNK), jnp.bfloat16),
    pltpu.VMEM((CHUNK, 256), jnp.float32),
    pltpu.VMEM((CHUNK, 256), jnp.float32),
    pltpu.VMEM((8, 256), jnp.float32),
    pltpu.VMEM((8, 256), jnp.float32),
]


def call(kernel, outs, scalars, arrays, flops, limit, scratch=(), aliases=None, places=None):
    return pl.pallas_call(
        kernel,
        out_shape=outs,
        in_specs=[SMEM] * len(scalars) + [VMEM] * len(arrays),
        out_specs=places or [VMEM] * len(outs),
        scratch_shapes=list(scratch),
        input_output_aliases=aliases or {},
        compiler_params=pltpu.CompilerParams(vmem_limit_bytes=limit * MIB),
        cost_estimate=pl.CostEstimate(flops=int(flops), bytes_accessed=10**6, transcendentals=0),
    )(*scalars, *arrays)


def layer(queries, keys, values, vertical, slash, out_weight):
    x, z, y, c = (lax.axis_index(a) for a in ALL)
    place = jnp.stack([x * 4 + z, y, jnp.where(c == 0, x, z), jnp.where(c == 0, z, x), c]).astype(jnp.int32)
    kv = call(kv_kernel, [bf16(SLAB, 256)] * 4, [place], [keys, values], 1e6, 4)
    kv = [kv[0]] + [along_y(kv[by], by) for by in (1, 2, 3)]
    q = call(q_kernel, [bf16(SLAB, 512)] * 4, [place], [queries], 1e6, 4)
    q = [q[0]] + [along_y(q[by], by) for by in (1, 2, 3)]
    table = call(table_kernel, [TABLE], [place, vertical, slash.T], [], 1e6, 4, (), None, [SMEM])[0]
    own, last = call(slots_kernel, [bf16(1024, 128), bf16(SLAB, 256)], [table], kv, 1e6, 4)
    hops = [first_hop(own, by) for by in (1, 2, 3)]
    prev = to_next_group(last)
    near = call(join_kernel, [bf16(4096, 128)], [], [own, *hops], 1e6, 4)[0]
    plus, minus = second_hop(near, 1), second_hop(near, 3)
    beyond = [second_hop(plus[:2048], 1), second_hop(minus[2048:], 3)]
    ql, *state, table = call(
        local_kernel, [bf16(16, 256, 128)] + PACKED + STATE + [TABLE], [table], [*q, *kv, prev, near], 3e9, 6,
        [pltpu.VMEM((5 * SLAB, 128), jnp.bfloat16)] * 2, None, [VMEM] * 6 + [SMEM],
    )
    state = call(
        functools.partial(part_kernel, 0, EVERY), PACKED + STATE, [table],
        [plus, minus, ql, *state], 1.5e10, 8, WORK, {4 + n: n for n in range(5)},
    )
    *state, a2, a1 = call(
        functools.partial(part_kernel, 1, (2, 1)), PACKED + STATE + [bf16(SLAB, 512)] * 2, [table],
        [*beyond, ql, *state], 3e9, 8, WORK, {4 + n: n for n in range(5)},
    )
    a2, a1 = along_y(a2, -2), along_y(a1, -1)
    *state, a3 = call(
        functools.partial(part_kernel, 2, (3,)), PACKED + STATE + [bf16(SLAB, 512)], [table],
        [ql, *state], 2e9, 8, WORK, {2 + n: n for n in range(5)},
    )
    a3 = along_y(a3, -3)
    *state, a0 = call(
        functools.partial(part_kernel, 2, (0,)), PACKED + STATE + [bf16(SLAB, 512)], [table],
        [ql, *state], 2e9, 8, WORK, {2 + n: n for n in range(5)},
    )
    total = call(early_kernel, [f32(SLAB, 4096)], [place], [a0, a1, a2, out_weight], 3e9, 6)[0]
    theirs, mine = (
        call(functools.partial(last_kernel, own), [out], [place], [a3, out_weight, total], 1e9, 6)[0]
        for own, out in ((False, bf16(128, 4096)), (True, f32(128, 4096)))
    )
    other = to_partner(theirs)
    return (mine + other.astype(jnp.float32)).astype(jnp.bfloat16)


def solution(mesh):
    torus = Mesh(mesh.devices.reshape(4, 4, 4, 2), ALL)
    rows = ("x", "z", "y")
    placed = (P(rows, "c"), P(rows, "c"), P(rows, "c"), P("c", None), P("c", None), P("c", None))
    return jax.shard_map(layer, mesh=torus, in_specs=placed, out_specs=P(ALL, None), check_vma=False)
```

```python
import functools

import jax
import jax.numpy as jnp
from jax import lax
from jax.experimental import pallas as pl
from jax.experimental.pallas import tpu as pltpu
from jax.sharding import Mesh
from jax.sharding import PartitionSpec as P

HEAD_DIM = 128
BLK = 64
SLAB = 256
NV = 64
EXP2_SCALE = HEAD_DIM ** (-0.5) * 1.4426950408889634
NEGATIVE = -1e30
SLASH = 8
VERT = 16
NEVER = 1 << 20
BOUNDS = 96
COUNTS = 128
ALL = ("x", "z", "y", "c")
MIB = 1 << 20


def moved(value, target):
    pairs = []
    for x in range(4):
        for z in range(4):
            for y in range(4):
                for c in range(2):
                    tx, tz, ty, tc = target(x, z, y, c)
                    pairs.append((((x * 4 + z) * 4 + y) * 2 + c, (((tx % 4) * 4 + tz % 4) * 4 + ty % 4) * 2 + tc))
    return lax.ppermute(value, ALL, pairs)


def along_y(value, by):
    return moved(value, lambda x, z, y, c: (x, z, y + by, c))


def first_hop(value, by):
    return moved(value, lambda x, z, y, c: (x + by, z, y, c) if c == 0 else (x, z + by, y, c))


def second_hop(value, by):
    return moved(value, lambda x, z, y, c: (x, z + by, y, c) if c == 0 else (x + by, z, y, c))


def to_next_group(value):
    return moved(value, lambda x, z, y, c: (x + (z + 1) // 4, z + 1, y, c))


def to_partner(value):
    return moved(value, lambda x, z, y, c: (x, z, y, 1 - c))


def row_rank(table_ref, block):
    at = jnp.int32(VERT)
    for width in (32, 16, 8, 4, 2, 1):
        at = at + jnp.where(table_ref[at + width - 1] < block, width, 0)
    return at - VERT + jnp.where(table_ref[at] < block, 1, 0)


def kv_kernel(place_ref, keys_ref, values_ref, *out_refs):
    y = place_ref[1]
    for by in range(4):
        lanes = pl.ds(pl.multiple_of((y + by) % 4 * HEAD_DIM, HEAD_DIM), HEAD_DIM)
        out_refs[by][:, 0:128] = keys_ref[:, lanes]
        out_refs[by][:, 128:256] = values_ref[:, lanes]


def q_kernel(place_ref, queries_ref, *out_refs):
    y = place_ref[1]
    for by in range(4):
        out_refs[by][...] = queries_ref[:, pl.ds(pl.multiple_of((y + by) % 4 * 512, 512), 512)]


def table_kernel(place_ref, vert_ref, slash_ref, table_ref):
    y = place_ref[1]
    for n in range(5):
        table_ref[n] = place_ref[n]
    for n in range(2):
        table_ref[SLASH + n] = slash_ref[n, y]
    for n in range(64):
        table_ref[COUNTS + n] = 0

    def one(n, carry):
        block = vert_ref[y, n]
        table_ref[VERT + n] = block
        slab = COUNTS + block // 4
        table_ref[slab] = table_ref[slab] + 1
        return carry

    lax.fori_loop(0, NV, one, 0)
    total = jnp.int32(0)
    for g in range(16):
        table_ref[BOUNDS + g] = total
        for n in range(4):
            total = total + table_ref[COUNTS + 4 * g + n]
    table_ref[BOUNDS + 16] = total


def slots_kernel(table_ref, kv0, kv1, kv2, kv3, own_ref, last_ref):
    group, y = table_ref[0], table_ref[1]
    for by, kv in enumerate((kv0, kv1, kv2, kv3)):
        slab = (y - by + 4) % 4
        first = (group * 4 + slab) * 4
        at = row_rank(table_ref, first)
        for slot in range(2):
            entry = jnp.minimum(at + slot, NV - 1)
            block = table_ref[VERT + entry] - first
            block = jnp.where((block >= 0) & (block < 4), block, 0)
            rows = pl.ds(pl.multiple_of(block * BLK, BLK), BLK)
            to = by * 256 + slot * BLK
            own_ref[to : to + BLK, :] = kv[rows, 0:128]
            own_ref[to + 128 : to + 128 + BLK, :] = kv[rows, 128:256]

        @pl.when(slab == 3)
        def _():
            last_ref[...] = kv[...]


def join_kernel(a0, a1, a2, a3, out_ref):
    for n, a in enumerate((a0, a1, a2, a3)):
        out_ref[n * 1024 : (n + 1) * 1024, :] = a[...]


CHUNK = 1024
HALF = 512
BIG = 2048
EVERY = (0, 1, 2, 3)


def scores_of(keys, q):
    return lax.dot_general(keys, q, (((1,), (1,)), ((), ())), preferred_element_type=jnp.float32)


def top_of(load, pieces):
    top = load(0)
    for t in range(1, pieces):
        top = jnp.maximum(top, load(t))
    eight = top[0:8]
    for r in range(1, 8):
        eight = jnp.maximum(eight, top[8 * r : 8 * r + 8])
    return eight


def weigh(i, load, pieces, eight, values, top, tot, acc, start=False):
    new = jnp.broadcast_to(jnp.max(eight, axis=0, keepdims=True), eight.shape)
    if not start:
        old = top[i]
        new = jnp.maximum(old, new)
    level = new[0:1]
    rounded, part = [], None
    for t in range(pieces):
        weights = jnp.exp2((load(t) - level) * EXP2_SCALE)
        for r in range(8):
            piece = weights[8 * r : 8 * r + 8]
            part = piece if part is None else part + piece
        rounded.append(weights.astype(jnp.bfloat16))
    product = jnp.dot(values, jnp.concatenate(rounded, axis=0), preferred_element_type=jnp.float32)
    top[i] = new
    if start:
        tot[i] = part
        acc[i] = product
        return
    shrink = jnp.exp2((old - new) * EXP2_SCALE)
    tot[i] = tot[i] * shrink + part
    acc[i] = acc[i] * shrink[0:1] + product


def block_of(place_ref, i):
    return place_ref[0] * 16 + ((place_ref[1] - i // 4 + 4) % 4) * 4 + i % 4


def group_at(table_ref, outer, inner):
    first = (table_ref[2] - inner + 4) % 4
    second = (table_ref[3] - outer + 4) % 4
    return jnp.where(table_ref[4] == 0, first * 4 + second, second * 4 + first)


def count_of(table_ref, outer):
    total = jnp.int32(0)
    for inner in range(4):
        g = group_at(table_ref, outer, inner)
        total = total + jnp.where(g < table_ref[0], table_ref[BOUNDS + g + 1] - table_ref[BOUNDS + g], 0)
    return total


def pack(table_ref, g, some, at, source, base, kc, vc):
    for n in range(4):
        row = pl.multiple_of((base * 4 + (table_ref[1] - n + 4) % 4) * 256, 256)
        rows = pl.ds(pl.multiple_of(at * BLK, BLK), 2 * BLK)
        kc[rows, :] = source[pl.ds(row, 128), :]
        vc[rows, :] = source[pl.ds(row + 128, 128), :]
        at = at + jnp.where(some, table_ref[COUNTS + 4 * g + n], 0)
    return at


def pack_all(table_ref, outer, at, sources, kc, vc):
    for inner in range(4):
        g = group_at(table_ref, outer, inner)
        part = 4 // len(sources)
        at = pack(table_ref, g, g < table_ref[0], at, sources[inner // part], inner % part, kc, vc)
    return at


def chunks(size, each, masked, picks, table_ref, order, begin, count, ql, kc, vc, top, tot, acc, vt_ref, sa_ref, sb_ref, ma, mb):
    pieces = size // BLK
    vt, sa, sb = vt_ref.at[:, 0:size], sa_ref.at[0:size, :], sb_ref.at[0:size, :]
    total = 4 * len(picks)
    steps = total // (2 * each)

    def query(m):
        if len(picks) == 4:
            return m
        if len(picks) == 1:
            return 4 * picks[0] + m
        return jnp.where(m < 4, 4 * picks[0], 4 * picks[1]) + m % 4

    def one_chunk(n, carry):
        first = begin + n * pieces
        rows = pl.ds(pl.multiple_of(first * BLK, HALF), size)
        vt[...] = vc[rows, :].T

        def score(i, buffer, eight):
            scores = scores_of(kc[rows, :], ql[i])
            if masked:
                mine = block_of(table_ref, i)
                scores = jnp.concatenate(
                    [
                        jnp.where(order[first + t] < mine, scores[BLK * t : BLK * (t + 1)], NEGATIVE)
                        for t in range(pieces)
                    ],
                    axis=0,
                )
            buffer[...] = scores
            eight[...] = top_of(lambda t: scores[BLK * t : BLK * (t + 1)], pieces)

        def finish(i, buffer, eight):
            weigh(i, lambda t: buffer[BLK * t : BLK * (t + 1), :], pieces, eight[...], vt[...], top, tot, acc)

        score(query(0), sa, ma)
        score(query(1), sb, mb)

        def some(j, carry):
            for u in range(each):
                m = 2 * (j * each + u)
                more = steps > 1 or u < each - 1
                finish(query(m), sa, ma)
                if more:
                    score(query((m + 2) % total), sa, ma)
                finish(query(m + 1), sb, mb)
                if more:
                    score(query((m + 3) % total), sb, mb)
            return carry

        if steps == 1:
            some(0, 0)
        else:
            lax.fori_loop(0, steps, some, 0)
        return carry

    lax.fori_loop(0, count, one_chunk, 0)


def part_kernel(stage, picks, table_ref, *refs):
    splits = ((1, 1), (2, 1), ())[stage]
    sources, refs = refs[: sum(splits)], refs[sum(splits) :]
    ql, refs = refs[0], refs[6:]
    kc, vc, top, tot, acc = refs[:5]
    outs, refs = (refs[5 : 5 + len(picks)], refs[5 + len(picks) :]) if stage else (None, refs[5:])
    order = refs[0]
    work = (ql, kc, vc, top, tot, acc, *refs[1:])
    others, total = table_ref[BOUNDS + table_ref[0]], table_ref[BOUNDS + table_ref[0] + 1]
    at = count_of(table_ref, 0)
    if stage == 0:
        at = pack_all(table_ref, 1, at, sources[:1], kc, vc)
        at = pack_all(table_ref, 3, at, sources[1:], kc, vc)
        chunks(BIG, 2, False, picks, table_ref, order, jnp.int32(0), at // 32, *work)
        chunks(CHUNK, 4, False, picks, table_ref, order, at // 32 * 32, at // 16 % 2, *work)
        return
    at = at + count_of(table_ref, 1) + count_of(table_ref, 3)
    begin = at // 16 * 16
    whole = (others - begin) // 16
    rest = begin + whole * 16
    long = (total - rest + 7) // 16
    short = (jnp.maximum(total - rest - 16 * long, 0) + 7) // 8
    end = rest + 16 * long + 8 * short
    if stage == 1:
        pack_all(table_ref, 2, at, sources[:2], kc, vc)
        pack(table_ref, table_ref[0], True, others, sources[2], 0, kc, vc)

    def mark(n, carry):
        own = table_ref[VERT + jnp.minimum(n, NV - 1)]
        order[n] = jnp.where(n < others, -1, jnp.where(n < total, own, NEVER))

        @pl.when(n >= total)
        def _():
            vc[pl.ds(pl.multiple_of(n * BLK, BLK), BLK), :] = jnp.zeros((BLK, 128), jnp.bfloat16)

        return carry

    lax.fori_loop(rest, end, mark, 0)
    chunks(CHUNK, 2 * len(picks), False, picks, table_ref, order, begin, whole, *work)
    chunks(CHUNK, 2 * len(picks), True, picks, table_ref, order, rest, long, *work)
    chunks(HALF, 2 * len(picks), True, picks, table_ref, order, rest + 16 * long, short, *work)
    for out, by in zip(outs, picks):
        for block in range(4):
            i = by * 4 + block
            o = (acc[i] / jnp.sum(tot[i], axis=0, keepdims=True)).T.astype(jnp.bfloat16)
            for g in range(4):
                out[block * BLK : (block + 1) * BLK, g * 128 : (g + 1) * 128] = o[g * BLK : (g + 1) * BLK, :]


def local_kernel(
    place_ref, q0, q1, q2, q3, kv0, kv1, kv2, kv3, prev_ref, near,
    ql, kc, vc, top, tot, acc, kl, vl
):
    group, y = place_ref[0], place_ref[1]
    kl[0:SLAB, :] = prev_ref[:, 0:128]
    vl[0:SLAB, :] = prev_ref[:, 128:256]
    for by, (q, kv) in enumerate(((q0, kv0), (q1, kv1), (q2, kv2), (q3, kv3))):
        slab = (y - by + 4) % 4
        rows = pl.ds(pl.multiple_of(SLAB + slab * SLAB, SLAB), SLAB)
        kl[rows, :] = kv[:, 0:128]
        vl[rows, :] = kv[:, 128:256]
        for block in range(4):
            for g in range(4):
                ql[by * 4 + block, g * BLK : (g + 1) * BLK, :] = q[block * BLK : (block + 1) * BLK, g * 128 : (g + 1) * 128]
    key = lax.broadcasted_iota(jnp.int32, (BLK, 256), 0)
    row = lax.broadcasted_iota(jnp.int32, (BLK, 256), 1) % BLK

    def some(j, carry):
        ready = []
        for u in range(4):
            i = 4 * j + u
            block = block_of(place_ref, i)
            here = block - group * 16
            starts, valid = [here], []
            for s in range(2):
                offset = place_ref[SLASH + s]
                behind = block - offset
                at = jnp.minimum(row_rank(place_ref, behind), NV - 1)
                valid.append((behind >= 0) & (place_ref[VERT + at] != behind))
                starts.append(here - offset)
            rows = [pl.ds(pl.multiple_of(SLAB + at * BLK, BLK), BLK) for at in starts]
            keys = jnp.concatenate([kl[r, :] for r in rows] + [kl[rows[0], :]], axis=0)
            values = jnp.concatenate([vl[r, :] for r in rows] + [vl[rows[0], :]], axis=0).T
            ready.append((i, scores_of(keys, ql[i]), values, valid))
        for i, scores, values, valid in ready:
            def load(t):
                if t == 3:
                    return jnp.full((BLK, 256), NEGATIVE, jnp.float32)
                here = scores[BLK * t : BLK * (t + 1)]
                return jnp.where(key <= row if t == 0 else valid[t - 1], here, NEGATIVE)

            weigh(i, load, 4, top_of(load, 4), values, top, tot, acc, True)
        return carry

    lax.fori_loop(0, 4, some, 0)
    pack_all(place_ref, 0, jnp.int32(0), [near], kc, vc)


def early_kernel(place_ref, a0, a1, a2, weight_ref, total_ref):
    for n in range(8):
        columns = slice(n * 512, (n + 1) * 512)
        total = None
        for by, a in enumerate((a0, a1, a2)):
            depth = pl.ds(pl.multiple_of((place_ref[1] + by) % 4 * 512, 512), 512)
            part = jnp.dot(a[...], weight_ref[depth, columns], preferred_element_type=jnp.float32)
            total = part if total is None else total + part
        total_ref[:, columns] = total


def last_kernel(mine, place_ref, a, weight_ref, total_ref, out_ref):
    core = place_ref[4]
    half = core if mine else 1 - core
    rows = pl.ds(pl.multiple_of(half * 128, 128), 128)
    depth = pl.ds(pl.multiple_of((place_ref[1] + 3) % 4 * 512, 512), 512)
    for n in range(8):
        columns = slice(n * 512, (n + 1) * 512)
        part = jnp.dot(a[rows, :], weight_ref[depth, columns], preferred_element_type=jnp.float32)
        out_ref[:, columns] = (total_ref[rows, columns] + part).astype(out_ref.dtype)


SMEM = pl.BlockSpec(memory_space=pltpu.SMEM)
VMEM = pl.BlockSpec(memory_space=pltpu.VMEM)


def bf16(*shape):
    return jax.ShapeDtypeStruct(shape, jnp.bfloat16)


def f32(*shape):
    return jax.ShapeDtypeStruct(shape, jnp.float32)


TABLE = jax.ShapeDtypeStruct((192,), jnp.int32)
STATE = [f32(16, 8, 256), f32(16, 8, 256), f32(16, 128, 256)]
PACKED = [bf16((NV + 2) * BLK, 128)] * 2


def work(size):
    return [
        pltpu.SMEM((NV + 16,), jnp.int32),
        pltpu.VMEM((128, size), jnp.bfloat16),
        pltpu.VMEM((size, 256), jnp.float32),
        pltpu.VMEM((size, 256), jnp.float32),
        pltpu.VMEM((8, 256), jnp.float32),
        pltpu.VMEM((8, 256), jnp.float32),
    ]


WORK, LONG = work(CHUNK), work(BIG)


def call(kernel, outs, scalars, arrays, flops, limit, scratch=(), aliases=None, places=None):
    return pl.pallas_call(
        kernel,
        out_shape=outs,
        in_specs=[SMEM] * len(scalars) + [VMEM] * len(arrays),
        out_specs=places or [VMEM] * len(outs),
        scratch_shapes=list(scratch),
        input_output_aliases=aliases or {},
        compiler_params=pltpu.CompilerParams(vmem_limit_bytes=limit * MIB),
        cost_estimate=pl.CostEstimate(flops=int(flops), bytes_accessed=10**6, transcendentals=0),
    )(*scalars, *arrays)


def layer(queries, keys, values, vertical, slash, out_weight):
    x, z, y, c = (lax.axis_index(a) for a in ALL)
    place = jnp.stack([x * 4 + z, y, jnp.where(c == 0, x, z), jnp.where(c == 0, z, x), c]).astype(jnp.int32)
    kv = call(kv_kernel, [bf16(SLAB, 256)] * 4, [place], [keys, values], 1e6, 4)
    kv = [kv[0]] + [along_y(kv[by], by) for by in (1, 2, 3)]
    q = call(q_kernel, [bf16(SLAB, 512)] * 4, [place], [queries], 1e6, 4)
    q = [q[0]] + [along_y(q[by], by) for by in (1, 2, 3)]
    table = call(table_kernel, [TABLE], [place, vertical, slash.T], [], 1e6, 4, (), None, [SMEM])[0]
    own, last = call(slots_kernel, [bf16(1024, 128), bf16(SLAB, 256)], [table], kv, 1e6, 4)
    hops = [first_hop(own, by) for by in (1, 2, 3)]
    prev = to_next_group(last)
    near = call(join_kernel, [bf16(4096, 128)], [], [own, *hops], 1e6, 4)[0]
    plus, minus = second_hop(near, 1), second_hop(near, 3)
    beyond = [second_hop(plus[:2048], 1), second_hop(minus[2048:], 3)]
    ql, *state = call(
        local_kernel, [bf16(16, 256, 128)] + PACKED + STATE, [table], [*q, *kv, prev, near], 3e9, 6,
        [pltpu.VMEM((5 * SLAB, 128), jnp.bfloat16)] * 2,
    )
    state = call(
        functools.partial(part_kernel, 0, EVERY), PACKED + STATE, [table],
        [plus, minus, ql, *state], 1.5e10, 10, LONG, {4 + n: n for n in range(5)},
    )
    *state, a2, a1 = call(
        functools.partial(part_kernel, 1, (2, 1)), PACKED + STATE + [bf16(SLAB, 512)] * 2, [table],
        [*beyond, near, ql, *state], 3e9, 8, WORK, {5 + n: n for n in range(5)},
    )
    a2, a1 = along_y(a2, -2), along_y(a1, -1)
    *state, a3 = call(
        functools.partial(part_kernel, 2, (3,)), PACKED + STATE + [bf16(SLAB, 512)], [table],
        [ql, *state], 2e9, 8, WORK, {2 + n: n for n in range(5)},
    )
    a3 = along_y(a3, -3)
    *state, a0 = call(
        functools.partial(part_kernel, 2, (0,)), PACKED + STATE + [bf16(SLAB, 512)], [table],
        [ql, *state], 2e9, 8, WORK, {2 + n: n for n in range(5)},
    )
    total = call(early_kernel, [f32(SLAB, 4096)], [place], [a0, a1, a2, out_weight], 3e9, 6)[0]
    theirs, mine = (
        call(functools.partial(last_kernel, own), [out], [place], [a3, out_weight, total], 1e9, 6)[0]
        for own, out in ((False, bf16(128, 4096)), (True, f32(128, 4096)))
    )
    other = to_partner(theirs)
    return (mine + other.astype(jnp.float32)).astype(jnp.bfloat16)


def solution(mesh):
    torus = Mesh(mesh.devices.reshape(4, 4, 4, 2), ALL)
    rows = ("x", "z", "y")
    placed = (P(rows, "c"), P(rows, "c"), P(rows, "c"), P("c", None), P("c", None), P("c", None))
    return jax.shard_map(layer, mesh=torus, in_specs=placed, out_specs=P(ALL, None), check_vma=False)
```

```python
import functools

import jax
import jax.numpy as jnp
from jax import lax
from jax.experimental import pallas as pl
from jax.experimental.pallas import tpu as pltpu
from jax.sharding import Mesh
from jax.sharding import PartitionSpec as P

HEAD_DIM = 128
BLK = 64
SLAB = 256
NV = 64
EXP2_SCALE = HEAD_DIM ** (-0.5) * 1.4426950408889634
NEGATIVE = -1e30
SLASH = 8
VERT = 16
NEVER = 1 << 20
BOUNDS = 96
COUNTS = 128
ALL = ("x", "z", "y", "c")
MIB = 1 << 20


def moved(value, target):
    pairs = []
    for x in range(4):
        for z in range(4):
            for y in range(4):
                for c in range(2):
                    tx, tz, ty, tc = target(x, z, y, c)
                    pairs.append((((x * 4 + z) * 4 + y) * 2 + c, (((tx % 4) * 4 + tz % 4) * 4 + ty % 4) * 2 + tc))
    return lax.ppermute(value, ALL, pairs)


def along_y(value, by):
    return moved(value, lambda x, z, y, c: (x, z, y + by, c))


def first_hop(value, by):
    return moved(value, lambda x, z, y, c: (x + by, z, y, c) if c == 0 else (x, z + by, y, c))


def second_hop(value, by):
    return moved(value, lambda x, z, y, c: (x, z + by, y, c) if c == 0 else (x + by, z, y, c))


def to_next_group(value):
    return moved(value, lambda x, z, y, c: (x + (z + 1) // 4, z + 1, y, c))


def to_partner(value):
    return moved(value, lambda x, z, y, c: (x, z, y, 1 - c))


def row_rank(table_ref, block):
    at = jnp.int32(VERT)
    for width in (32, 16, 8, 4, 2, 1):
        at = at + jnp.where(table_ref[at + width - 1] < block, width, 0)
    return at - VERT + jnp.where(table_ref[at] < block, 1, 0)


def kv_kernel(place_ref, keys, values, o0, o1, o2, o3, sems):
    moves = []
    for by, out in enumerate((o0, o1, o2, o3)):
        lanes = pl.ds(pl.multiple_of((place_ref[1] + by) % 4 * HEAD_DIM, HEAD_DIM), HEAD_DIM)
        moves.append(pltpu.make_async_copy(keys.at[:, lanes], out.at[:, 0:128], sems.at[2 * by]))
        moves.append(pltpu.make_async_copy(values.at[:, lanes], out.at[:, 128:256], sems.at[2 * by + 1]))
    for move in moves:
        move.start()
    for move in moves:
        move.wait()


def q_kernel(place_ref, queries_ref, *out_refs):
    y = place_ref[1]
    for by in range(4):
        out_refs[by][...] = queries_ref[:, pl.ds(pl.multiple_of((y + by) % 4 * 512, 512), 512)]


def table_kernel(place_ref, vert_ref, slash_ref, table_ref):
    y = place_ref[1]
    for n in range(5):
        table_ref[n] = place_ref[n]
    for n in range(2):
        table_ref[SLASH + n] = slash_ref[n, y]
    for n in range(64):
        table_ref[COUNTS + n] = 0

    def one(n, carry):
        block = vert_ref[y, n]
        table_ref[VERT + n] = block
        slab = COUNTS + block // 4
        table_ref[slab] = table_ref[slab] + 1
        return carry

    lax.fori_loop(0, NV, one, 0)
    total = jnp.int32(0)
    for g in range(16):
        table_ref[BOUNDS + g] = total
        for n in range(4):
            total = total + table_ref[COUNTS + 4 * g + n]
    table_ref[BOUNDS + 16] = total


def slots_kernel(table_ref, kv0, kv1, kv2, kv3, own_ref, last_ref):
    group, y = table_ref[0], table_ref[1]
    for by, kv in enumerate((kv0, kv1, kv2, kv3)):
        slab = (y - by + 4) % 4
        first = (group * 4 + slab) * 4
        at = row_rank(table_ref, first)
        for slot in range(2):
            entry = jnp.minimum(at + slot, NV - 1)
            block = table_ref[VERT + entry] - first
            block = jnp.where((block >= 0) & (block < 4), block, 0)
            rows = pl.ds(pl.multiple_of(block * BLK, BLK), BLK)
            to = by * 256 + slot * BLK
            own_ref[to : to + BLK, :] = kv[rows, 0:128]
            own_ref[to + 128 : to + 128 + BLK, :] = kv[rows, 128:256]

        @pl.when(slab == 3)
        def _():
            last_ref[...] = kv[...]


def join_kernel(a0, a1, a2, a3, out_ref):
    for n, a in enumerate((a0, a1, a2, a3)):
        out_ref[n * 1024 : (n + 1) * 1024, :] = a[...]


CHUNK = 1024
HALF = 512
BIG = 2048
EVERY = (0, 1, 2, 3)


def scores_of(keys, q):
    return lax.dot_general(keys, q, (((1,), (1,)), ((), ())), preferred_element_type=jnp.float32)


def top_of(load, pieces):
    top = load(0)
    for t in range(1, pieces):
        top = jnp.maximum(top, load(t))
    eight = top[0:8]
    for r in range(1, 8):
        eight = jnp.maximum(eight, top[8 * r : 8 * r + 8])
    return eight


def weigh(i, load, pieces, eight, values, top, tot, acc, start=False):
    new = jnp.broadcast_to(jnp.max(eight, axis=0, keepdims=True), eight.shape)
    if not start:
        old = top[i]
        new = jnp.maximum(old, new)
    level = new[0:1]
    rounded, part = [], None
    for t in range(pieces):
        weights = jnp.exp2((load(t) - level) * EXP2_SCALE)
        for r in range(8):
            piece = weights[8 * r : 8 * r + 8]
            part = piece if part is None else part + piece
        rounded.append(weights.astype(jnp.bfloat16))
    product = jnp.dot(values, jnp.concatenate(rounded, axis=0), preferred_element_type=jnp.float32)
    top[i] = new
    if start:
        tot[i] = part
        acc[i] = product
        return
    shrink = jnp.exp2((old - new) * EXP2_SCALE)
    tot[i] = tot[i] * shrink + part
    acc[i] = acc[i] * shrink[0:1] + product


def block_of(place_ref, i):
    return place_ref[0] * 16 + ((place_ref[1] - i // 4 + 4) % 4) * 4 + i % 4


def group_at(table_ref, outer, inner):
    first = (table_ref[2] - inner + 4) % 4
    second = (table_ref[3] - outer + 4) % 4
    return jnp.where(table_ref[4] == 0, first * 4 + second, second * 4 + first)


def count_of(table_ref, outer):
    total = jnp.int32(0)
    for inner in range(4):
        g = group_at(table_ref, outer, inner)
        total = total + jnp.where(g < table_ref[0], table_ref[BOUNDS + g + 1] - table_ref[BOUNDS + g], 0)
    return total


def pack(table_ref, g, some, at, source, base, kc, vc):
    for n in range(4):
        row = pl.multiple_of((base * 4 + (table_ref[1] - n + 4) % 4) * 256, 256)
        rows = pl.ds(pl.multiple_of(at * BLK, BLK), 2 * BLK)
        kc[rows, :] = source[pl.ds(row, 128), :]
        vc[rows, :] = source[pl.ds(row + 128, 128), :]
        at = at + jnp.where(some, table_ref[COUNTS + 4 * g + n], 0)
    return at


def pack_all(table_ref, outer, at, sources, kc, vc):
    for inner in range(4):
        g = group_at(table_ref, outer, inner)
        part = 4 // len(sources)
        at = pack(table_ref, g, g < table_ref[0], at, sources[inner // part], inner % part, kc, vc)
    return at


def chunks(size, each, masked, picks, table_ref, order, begin, count, ql, kc, vc, top, tot, acc, vt_ref, sa_ref, sb_ref, ma, mb):
    pieces = size // BLK
    vt, sa, sb = vt_ref.at[:, 0:size], sa_ref.at[0:size, :], sb_ref.at[0:size, :]
    total = 4 * len(picks)
    steps = total // (2 * each)

    def query(m):
        if len(picks) == 4:
            return m
        if len(picks) == 1:
            return 4 * picks[0] + m
        return jnp.where(m < 4, 4 * picks[0], 4 * picks[1]) + m % 4

    def one_chunk(n, carry):
        first = begin + n * pieces
        rows = pl.ds(pl.multiple_of(first * BLK, HALF), size)
        vt[...] = vc[rows, :].T

        def score(i, buffer, eight):
            scores = scores_of(kc[rows, :], ql[i])
            if masked:
                mine = block_of(table_ref, i)
                scores = jnp.concatenate(
                    [
                        jnp.where(order[first + t] < mine, scores[BLK * t : BLK * (t + 1)], NEGATIVE)
                        for t in range(pieces)
                    ],
                    axis=0,
                )
            buffer[...] = scores
            eight[...] = top_of(lambda t: scores[BLK * t : BLK * (t + 1)], pieces)

        def finish(i, buffer, eight):
            weigh(i, lambda t: buffer[BLK * t : BLK * (t + 1), :], pieces, eight[...], vt[...], top, tot, acc)

        score(query(0), sa, ma)
        score(query(1), sb, mb)

        def some(j, carry):
            for u in range(each):
                m = 2 * (j * each + u)
                more = steps > 1 or u < each - 1
                finish(query(m), sa, ma)
                if more:
                    score(query((m + 2) % total), sa, ma)
                finish(query(m + 1), sb, mb)
                if more:
                    score(query((m + 3) % total), sb, mb)
            return carry

        if steps == 1:
            some(0, 0)
        else:
            lax.fori_loop(0, steps, some, 0)
        return carry

    lax.fori_loop(0, count, one_chunk, 0)


def part_kernel(stage, picks, table_ref, *refs):
    splits = ((1, 1), (2, 1), ())[stage]
    sources, refs = refs[: sum(splits)], refs[sum(splits) :]
    ql, refs = refs[0], refs[6:]
    kc, vc, top, tot, acc = refs[:5]
    outs, refs = (refs[5 : 5 + len(picks)], refs[5 + len(picks) :]) if stage else (None, refs[5:])
    order = refs[0]
    work = (ql, kc, vc, top, tot, acc, *refs[1:])
    others, total = table_ref[BOUNDS + table_ref[0]], table_ref[BOUNDS + table_ref[0] + 1]
    at = count_of(table_ref, 0)
    if stage == 0:
        at = pack_all(table_ref, 1, at, sources[:1], kc, vc)
        at = pack_all(table_ref, 3, at, sources[1:], kc, vc)
        chunks(BIG, 2, False, picks, table_ref, order, jnp.int32(0), at // 32, *work)
        chunks(CHUNK, 4, False, picks, table_ref, order, at // 32 * 32, at // 16 % 2, *work)
        return
    at = at + count_of(table_ref, 1) + count_of(table_ref, 3)
    begin = at // 16 * 16
    whole = (others - begin) // 16
    rest = begin + whole * 16
    long = (total - rest + 7) // 16
    short = (jnp.maximum(total - rest - 16 * long, 0) + 7) // 8
    end = rest + 16 * long + 8 * short
    if stage == 1:
        pack_all(table_ref, 2, at, sources[:2], kc, vc)
        pack(table_ref, table_ref[0], True, others, sources[2], 0, kc, vc)

    def mark(n, carry):
        own = table_ref[VERT + jnp.minimum(n, NV - 1)]
        order[n] = jnp.where(n < others, -1, jnp.where(n < total, own, NEVER))

        @pl.when(n >= total)
        def _():
            vc[pl.ds(pl.multiple_of(n * BLK, BLK), BLK), :] = jnp.zeros((BLK, 128), jnp.bfloat16)

        return carry

    lax.fori_loop(rest, end, mark, 0)
    chunks(CHUNK, 2 * len(picks), False, picks, table_ref, order, begin, whole, *work)
    chunks(CHUNK, 2 * len(picks), True, picks, table_ref, order, rest, long, *work)
    chunks(HALF, 2 * len(picks), True, picks, table_ref, order, rest + 16 * long, short, *work)
    for out, by in zip(outs, picks):
        for block in range(4):
            i = by * 4 + block
            o = (acc[i] / jnp.sum(tot[i], axis=0, keepdims=True)).T.astype(jnp.bfloat16)
            for g in range(4):
                out[block * BLK : (block + 1) * BLK, g * 128 : (g + 1) * 128] = o[g * BLK : (g + 1) * BLK, :]


def local_kernel(
    place_ref, q0, q1, q2, q3, kv0, kv1, kv2, kv3, prev_ref, near,
    ql, kc, vc, top, tot, acc, kl, vl
):
    group, y = place_ref[0], place_ref[1]
    kl[0:SLAB, :] = prev_ref[:, 0:128]
    vl[0:SLAB, :] = prev_ref[:, 128:256]
    for by, (q, kv) in enumerate(((q0, kv0), (q1, kv1), (q2, kv2), (q3, kv3))):
        slab = (y - by + 4) % 4
        rows = pl.ds(pl.multiple_of(SLAB + slab * SLAB, SLAB), SLAB)
        kl[rows, :] = kv[:, 0:128]
        vl[rows, :] = kv[:, 128:256]
        for block in range(4):
            for g in range(4):
                ql[by * 4 + block, g * BLK : (g + 1) * BLK, :] = q[block * BLK : (block + 1) * BLK, g * 128 : (g + 1) * 128]
    key = lax.broadcasted_iota(jnp.int32, (BLK, 256), 0)
    row = lax.broadcasted_iota(jnp.int32, (BLK, 256), 1) % BLK

    def some(j, carry):
        ready = []
        for u in range(4):
            i = 4 * j + u
            block = block_of(place_ref, i)
            here = block - group * 16
            starts, valid = [here], []
            for s in range(2):
                offset = place_ref[SLASH + s]
                behind = block - offset
                at = jnp.minimum(row_rank(place_ref, behind), NV - 1)
                valid.append((behind >= 0) & (place_ref[VERT + at] != behind))
                starts.append(here - offset)
            rows = [pl.ds(pl.multiple_of(SLAB + at * BLK, BLK), BLK) for at in starts]
            keys = jnp.concatenate([kl[r, :] for r in rows] + [kl[rows[0], :]], axis=0)
            values = jnp.concatenate([vl[r, :] for r in rows] + [vl[rows[0], :]], axis=0).T
            ready.append((i, scores_of(keys, ql[i]), values, valid))
        for i, scores, values, valid in ready:
            def load(t):
                if t == 3:
                    return jnp.full((BLK, 256), NEGATIVE, jnp.float32)
                here = scores[BLK * t : BLK * (t + 1)]
                return jnp.where(key <= row if t == 0 else valid[t - 1], here, NEGATIVE)

            weigh(i, load, 4, top_of(load, 4), values, top, tot, acc, True)
        return carry

    lax.fori_loop(0, 4, some, 0)
    pack_all(place_ref, 0, jnp.int32(0), [near], kc, vc)


def early_kernel(place_ref, a0, a1, a2, weight_ref, total_ref):
    for n in range(8):
        columns = slice(n * 512, (n + 1) * 512)
        total = None
        for by, a in enumerate((a0, a1, a2)):
            depth = pl.ds(pl.multiple_of((place_ref[1] + by) % 4 * 512, 512), 512)
            part = jnp.dot(a[...], weight_ref[depth, columns], preferred_element_type=jnp.float32)
            total = part if total is None else total + part
        total_ref[:, columns] = total


def last_kernel(mine, place_ref, a, weight_ref, total_ref, out_ref):
    core = place_ref[4]
    half = core if mine else 1 - core
    rows = pl.ds(pl.multiple_of(half * 128, 128), 128)
    depth = pl.ds(pl.multiple_of((place_ref[1] + 3) % 4 * 512, 512), 512)
    for n in range(8):
        columns = slice(n * 512, (n + 1) * 512)
        part = jnp.dot(a[rows, :], weight_ref[depth, columns], preferred_element_type=jnp.float32)
        out_ref[:, columns] = (total_ref[rows, columns] + part).astype(out_ref.dtype)


SMEM = pl.BlockSpec(memory_space=pltpu.SMEM)
VMEM = pl.BlockSpec(memory_space=pltpu.VMEM)
HBM = pl.BlockSpec(memory_space=pltpu.HBM)
LIMIT = 54900


def bf16(*shape):
    return jax.ShapeDtypeStruct(shape, jnp.bfloat16)


def f32(*shape):
    return jax.ShapeDtypeStruct(shape, jnp.float32)


TABLE = jax.ShapeDtypeStruct((192,), jnp.int32)
STATE = [f32(16, 8, 256), f32(16, 8, 256), f32(16, 128, 256)]
PACKED = [bf16((NV + 2) * BLK, 128)] * 2


def work(size):
    return [
        pltpu.SMEM((NV + 16,), jnp.int32),
        pltpu.VMEM((128, size), jnp.bfloat16),
        pltpu.VMEM((size, 256), jnp.float32),
        pltpu.VMEM((size, 256), jnp.float32),
        pltpu.VMEM((8, 256), jnp.float32),
        pltpu.VMEM((8, 256), jnp.float32),
    ]


WORK, LONG = work(CHUNK), work(BIG)


def call(kernel, outs, scalars, arrays, flops, limit, scratch=(), aliases=None, places=None):
    return pl.pallas_call(
        kernel,
        out_shape=outs,
        in_specs=[SMEM] * len(scalars) + [VMEM] * len(arrays),
        out_specs=places or [VMEM] * len(outs),
        scratch_shapes=list(scratch),
        input_output_aliases=aliases or {},
        compiler_params=pltpu.CompilerParams(vmem_limit_bytes=limit * MIB),
        cost_estimate=pl.CostEstimate(flops=int(flops), bytes_accessed=10**6, transcendentals=0),
    )(*scalars, *arrays)


def layer(queries, keys, values, vertical, slash, out_weight):
    x, z, y, c = (lax.axis_index(a) for a in ALL)
    place = jnp.stack([x * 4 + z, y, jnp.where(c == 0, x, z), jnp.where(c == 0, z, x), c]).astype(jnp.int32)
    kv = pl.pallas_call(
        kv_kernel,
        out_shape=[bf16(SLAB, 256)] * 4,
        in_specs=[SMEM, HBM, HBM],
        out_specs=[VMEM] * 4,
        scratch_shapes=[pltpu.SemaphoreType.DMA((8,))],
        compiler_params=pltpu.CompilerParams(vmem_limit_bytes=LIMIT * 1024),
        name="kv",
    )(place, keys, values)
    kv = [kv[0]] + [along_y(kv[by], by) for by in (1, 2, 3)]
    q = call(q_kernel, [bf16(SLAB, 512)] * 4, [place], [queries], 1e6, 4)
    q = [q[0]] + [along_y(q[by], by) for by in (1, 2, 3)]
    table = call(table_kernel, [TABLE], [place, vertical, slash.T], [], 1e6, 4, (), None, [SMEM])[0]
    own, last = call(slots_kernel, [bf16(1024, 128), bf16(SLAB, 256)], [table], kv, 1e6, 4)
    hops = [first_hop(own, by) for by in (1, 2, 3)]
    prev = to_next_group(last)
    near = call(join_kernel, [bf16(4096, 128)], [], [own, *hops], 1e6, 4)[0]
    plus, minus = second_hop(near, 1), second_hop(near, 3)
    beyond = [second_hop(plus[:2048], 1), second_hop(minus[2048:], 3)]
    ql, *state = call(
        local_kernel, [bf16(16, 256, 128)] + PACKED + STATE, [table], [*q, *kv, prev, near], 3e9, 6,
        [pltpu.VMEM((5 * SLAB, 128), jnp.bfloat16)] * 2,
    )
    state = call(
        functools.partial(part_kernel, 0, EVERY), PACKED + STATE, [table],
        [plus, minus, ql, *state], 1.5e10, 10, LONG, {4 + n: n for n in range(5)},
    )
    *state, a2, a1 = call(
        functools.partial(part_kernel, 1, (2, 1)), PACKED + STATE + [bf16(SLAB, 512)] * 2, [table],
        [*beyond, near, ql, *state], 3e9, 8, WORK, {5 + n: n for n in range(5)},
    )
    a2, a1 = along_y(a2, -2), along_y(a1, -1)
    *state, a3 = call(
        functools.partial(part_kernel, 2, (3,)), PACKED + STATE + [bf16(SLAB, 512)], [table],
        [ql, *state], 2e9, 8, WORK, {2 + n: n for n in range(5)},
    )
    a3 = along_y(a3, -3)
    *state, a0 = call(
        functools.partial(part_kernel, 2, (0,)), PACKED + STATE + [bf16(SLAB, 512)], [table],
        [ql, *state], 2e9, 8, WORK, {2 + n: n for n in range(5)},
    )
    total = call(early_kernel, [f32(SLAB, 4096)], [place], [a0, a1, a2, out_weight], 3e9, 6)[0]
    theirs, mine = (
        call(functools.partial(last_kernel, own), [out], [place], [a3, out_weight, total], 1e9, 6)[0]
        for own, out in ((False, bf16(128, 4096)), (True, f32(128, 4096)))
    )
    other = to_partner(theirs)
    return (mine + other.astype(jnp.float32)).astype(jnp.bfloat16)


def solution(mesh):
    torus = Mesh(mesh.devices.reshape(4, 4, 4, 2), ALL)
    rows = ("x", "z", "y")
    placed = (P(rows, "c"), P(rows, "c"), P(rows, "c"), P("c", None), P("c", None), P("c", None))
    return jax.shard_map(layer, mesh=torus, in_specs=placed, out_specs=P(ALL, None), check_vma=False)
```
